32 devices in a mesh: dp: 4 (over x, y), tp: 8 (over z, core).
Axes of the slice: x: 2, y: 2, z: 4, core: 2. Of those that a mesh axis runs over, the one named last changes fastest.
Arguments:
- tokens: int32 [64], P('dp'), parts along dimension 0
- positions: int32 [64], P('dp'), parts along dimension 0
- self_keys: bfloat16 [2, 64, 448, 16, 64], P(None, 'dp', None, 'tp'), parts along dimension 1
- self_vals: bfloat16 [2, 64, 448, 16, 64], P(None, 'dp', None, 'tp'), parts along dimension 1
- cross_keys: bfloat16 [2, 64, 1500, 16, 64], P(None, 'dp', None, 'tp'), parts along dimension 1
- cross_vals: bfloat16 [2, 64, 1500, 16, 64], P(None, 'dp', None, 'tp'), parts along dimension 1
- embed_table: bfloat16 [52224, 1024], P('tp')
- pos_table: bfloat16 [448, 1024], replicated
- w_qkv: bfloat16 [2, 1024, 3, 16, 64], P(None, None, None, 'tp')
- w_cq: bfloat16 [2, 1024, 16, 64], P(None, None, 'tp')
- in_bias: float32 [2, 3, 16, 64], P(None, None, 'tp')
- w_out: bfloat16 [2, 2, 16, 64, 1024], P(None, None, 'tp')
- out_bias: float32 [2, 3, 1024], replicated
- w_fc1: bfloat16 [2, 1024, 4096], P(None, None, 'tp')
- b_fc1: float32 [2, 4096], P(None, 'tp')
- w_fc2: bfloat16 [2, 4096, 1024], P(None, 'tp')
- ln_layers: float32 [2, 3, 2, 1024], replicated
- ln_final: float32 [2, 1024], replicated
Outputs:
- output 1: float32 [64, 52224], P('dp', 'tp'), parts along dimension 0
- output 2: bfloat16 [2, 64, 448, 16, 64], P(None, 'dp', None, 'tp'), parts along dimension 1
- output 3: bfloat16 [2, 64, 448, 16, 64], P(None, 'dp', None, 'tp'), parts along dimension 1
There are 4 independent parts. The reference program is written for one: setup_inputs(seed, part) draws one part's arguments, and reference() takes and returns one part's arrays. A program takes and returns all parts, laid end to end along the dimension named above; an argument that names none is the same for every part.
All inputs are finite; a program needn't handle non-finite values.
Results may differ from the reference program's by a relative error of at most 0.0123359.
Values are sent between devices in bfloat16 or wider.
A program may use at most 1 GiB of HBM per device.

```python
import jax
import jax.numpy as jnp
from jax import lax

SEQ_BATCH = 16
D_MODEL = 1024
N_HEADS = 16
HEAD_DIM = 64
FF_DIM = 4096
VOCAB_SIZE = 51865
VOCAB_PAD = 52224
TEXT_CTX = 448
FRAMES = 1500
LAYERS = 2
FRAME_RANK = 8


def setup_inputs(seed: int = 0, part: int = 0) -> dict:
    base_key = jax.random.key(seed)
    part_keys = jax.random.split(jax.random.fold_in(base_key, part), 12)
    shared_keys = jax.random.split(jax.random.fold_in(base_key, 1000003), 14)

    def normal_draw(key_in, draw_shape, factor):
        return jax.random.normal(key_in, draw_shape, jnp.float32) * factor

    def structured(code_key, basis_key, noise_key, length, factor, noise_std):
        frame_codes = normal_draw(code_key, (SEQ_BATCH, length, FRAME_RANK), 1.0)
        code_basis = normal_draw(basis_key, (LAYERS, SEQ_BATCH, FRAME_RANK, N_HEADS, HEAD_DIM), factor * FRAME_RANK ** -0.5)
        mixed_rows = jnp.einsum('btr,lbrhe->lbthe', frame_codes, code_basis)
        return mixed_rows + normal_draw(noise_key, (LAYERS, SEQ_BATCH, length, N_HEADS, HEAD_DIM), noise_std)

    tokens = jax.random.randint(part_keys[0], (SEQ_BATCH,), 0, VOCAB_SIZE, dtype=jnp.int32)
    tokens = tokens.at[0].set(VOCAB_SIZE - 1).at[1].set(0)
    positions = jax.random.randint(part_keys[1], (SEQ_BATCH,), 0, TEXT_CTX, dtype=jnp.int32)
    positions = positions.at[0].set(TEXT_CTX - 1).at[1].set(0)
    self_keys = structured(part_keys[2], part_keys[3], part_keys[4], TEXT_CTX, 1.0, 0.3).astype(jnp.bfloat16)
    self_vals = structured(part_keys[2], part_keys[5], part_keys[6], TEXT_CTX, 1.0, 0.5).astype(jnp.bfloat16)
    cross_keys = structured(part_keys[7], part_keys[8], part_keys[9], FRAMES, 1.0, 0.3).astype(jnp.bfloat16)
    cross_vals = structured(part_keys[7], part_keys[10], part_keys[11], FRAMES, 1.0, 0.5).astype(jnp.bfloat16)
    embed_table = normal_draw(shared_keys[12], (VOCAB_PAD, D_MODEL), D_MODEL ** -0.25).astype(jnp.bfloat16)
    pos_table = normal_draw(shared_keys[13], (TEXT_CTX, D_MODEL), 0.5).astype(jnp.bfloat16)
    w_qkv = normal_draw(shared_keys[0], (LAYERS, D_MODEL, 3, N_HEADS, HEAD_DIM), D_MODEL ** -0.5).astype(jnp.bfloat16)
    w_cq = normal_draw(shared_keys[1], (LAYERS, D_MODEL, N_HEADS, HEAD_DIM), D_MODEL ** -0.5).astype(jnp.bfloat16)
    in_bias = normal_draw(shared_keys[2], (LAYERS, 3, N_HEADS, HEAD_DIM), 0.3)
    w_out = normal_draw(shared_keys[3], (LAYERS, 2, N_HEADS, HEAD_DIM, D_MODEL), D_MODEL ** -0.5).astype(jnp.bfloat16)
    out_bias = normal_draw(shared_keys[4], (LAYERS, 3, D_MODEL), 0.3)
    w_fc1 = normal_draw(shared_keys[5], (LAYERS, D_MODEL, FF_DIM), D_MODEL ** -0.5).astype(jnp.bfloat16)
    b_fc1 = normal_draw(shared_keys[6], (LAYERS, FF_DIM), 0.3)
    w_fc2 = normal_draw(shared_keys[7], (LAYERS, FF_DIM, D_MODEL), FF_DIM ** -0.5).astype(jnp.bfloat16)
    ln_layers = jnp.concatenate([1.0 + normal_draw(shared_keys[8], (LAYERS, 3, 1, D_MODEL), 0.2), normal_draw(shared_keys[9], (LAYERS, 3, 1, D_MODEL), 0.2)], axis=2)
    ln_final = jnp.concatenate([1.0 + normal_draw(shared_keys[10], (1, D_MODEL), 0.2), normal_draw(shared_keys[11], (1, D_MODEL), 0.2)], axis=0)
    return {'tokens': tokens, 'positions': positions, 'self_keys': self_keys, 'self_vals': self_vals, 'cross_keys': cross_keys, 'cross_vals': cross_vals, 'embed_table': embed_table, 'pos_table': pos_table, 'w_qkv': w_qkv, 'w_cq': w_cq, 'in_bias': in_bias, 'w_out': w_out, 'out_bias': out_bias, 'w_fc1': w_fc1, 'b_fc1': b_fc1, 'w_fc2': w_fc2, 'ln_layers': ln_layers, 'ln_final': ln_final}


def layer_norm(resid_in, ln_gain, ln_shift):
    row_mean = jnp.mean(resid_in, axis=-1, keepdims=True)
    centred = resid_in - row_mean
    variance = jnp.mean(centred * centred, axis=-1, keepdims=True)
    return (centred * lax.rsqrt(variance + 1e-5) * ln_gain + ln_shift).astype(jnp.bfloat16)


def attend(queries, key_rows, val_rows, mask_add):
    scores = jnp.einsum('bhe,bthe->bht', queries.astype(jnp.float32), key_rows.astype(jnp.float32)) * (HEAD_DIM ** -0.5) + mask_add
    weights = jax.nn.softmax(scores, axis=-1).astype(jnp.bfloat16)
    mixed_vals = jnp.einsum('bht,bthe->bhe', weights.astype(jnp.float32), val_rows.astype(jnp.float32))
    return mixed_vals.astype(jnp.bfloat16)


def project_out(attended, out_weight):
    summed = jnp.einsum('bhe,hed->bd', attended.astype(jnp.float32), out_weight.astype(jnp.float32))
    return summed.astype(jnp.bfloat16).astype(jnp.float32)


def reference(tokens, positions, self_keys, self_vals, cross_keys, cross_vals, embed_table, pos_table, w_qkv, w_cq, in_bias, w_out, out_bias, w_fc1, b_fc1, w_fc2, ln_layers, ln_final):
    residual = embed_table[tokens].astype(jnp.float32) + pos_table[positions].astype(jnp.float32)
    cache_pos = jnp.arange(TEXT_CTX)[None, :]
    write_mask = (cache_pos == positions[:, None])[:, :, None, None]
    self_mask = jnp.where(cache_pos <= positions[:, None], 0.0, -1e30)[:, None, :]

    def layer_body(resid_in, layer_args):
        (cache_keys, cache_vals, frame_keys, frame_vals, qkv_weight, cq_weight, bias_in, out_weight, bias_out, fc1_weight, fc1_bias, fc2_weight, ln_params) = layer_args
        hidden = layer_norm(resid_in, ln_params[0, 0], ln_params[0, 1])
        projected = jnp.einsum('bd,dthe->bthe', hidden.astype(jnp.float32), qkv_weight.astype(jnp.float32))
        queries = (projected[:, 0] + bias_in[0]).astype(jnp.bfloat16)
        key_new = projected[:, 1].astype(jnp.bfloat16)
        val_new = (projected[:, 2] + bias_in[1]).astype(jnp.bfloat16)
        keys_now = jnp.where(write_mask, key_new[:, None], cache_keys)
        vals_now = jnp.where(write_mask, val_new[:, None], cache_vals)
        resid_mid = resid_in + project_out(attend(queries, keys_now, vals_now, self_mask), out_weight[0]) + bias_out[0]
        hidden = layer_norm(resid_mid, ln_params[1, 0], ln_params[1, 1])
        cross_q = (jnp.einsum('bd,dhe->bhe', hidden.astype(jnp.float32), cq_weight.astype(jnp.float32)) + bias_in[2]).astype(jnp.bfloat16)
        resid_mid = resid_mid + project_out(attend(cross_q, frame_keys, frame_vals, 0.0), out_weight[1]) + bias_out[1]
        hidden = layer_norm(resid_mid, ln_params[2, 0], ln_params[2, 1])
        fc1_out = jnp.dot(hidden, fc1_weight, preferred_element_type=jnp.float32) + fc1_bias
        active = jax.nn.gelu(fc1_out, approximate=False).astype(jnp.bfloat16)
        fc2_out = jnp.dot(active, fc2_weight, preferred_element_type=jnp.float32).astype(jnp.bfloat16).astype(jnp.float32)
        resid_out = resid_mid + fc2_out + bias_out[2]
        return resid_out, (keys_now, vals_now)

    residual, new_caches = lax.scan(layer_body, residual, (self_keys, self_vals, cross_keys, cross_vals, w_qkv, w_cq, in_bias, w_out, out_bias, w_fc1, b_fc1, w_fc2, ln_layers))
    final_hidden = layer_norm(residual, ln_final[0], ln_final[1])
    logits = jnp.dot(final_hidden, embed_table.T, preferred_element_type=jnp.float32)
    return logits, new_caches[0], new_caches[1]
```

```python
import functools

import jax
import jax.numpy as jnp
from jax import lax
from jax.experimental import pallas as pl
from jax.experimental.pallas import tpu as pltpu
from jax.sharding import PartitionSpec as P

BF16 = jnp.bfloat16
F32 = jnp.float32
MESH = pl.DeviceIdType.MESH
N_TP = 8
OWNERS = (3, 5)
ROWS = 8
BATCH = 16
HEADS = 2
HEAD_DIM = 64
HD = HEADS * HEAD_DIM
LAYERS = 2
N_PHASES = 1 + 3 * LAYERS
NEG = -1e30


def dot(a, b):
    return jnp.dot(a, b, preferred_element_type=F32)


def dot_nt(a, b):
    return lax.dot_general(a, b, (((1,), (1,)), ((), ())), preferred_element_type=F32)


def layer_norm(x, gain, shift):
    mean = jnp.mean(x, axis=-1, keepdims=True)
    centred = x - mean
    var = jnp.mean(centred * centred, axis=-1, keepdims=True)
    return (centred * lax.rsqrt(var + 1e-5) * gain + shift).astype(BF16)


def head_row(ref, *idx):
    v = ref[idx]
    return jnp.concatenate([v[0:1], v[1:2]], axis=1)


def spread_queries(q):
    q2 = jnp.concatenate([q, q], axis=0)
    row = lax.broadcasted_iota(jnp.int32, (2 * BATCH, HD), 0)
    lane = lax.broadcasted_iota(jnp.int32, (2 * BATCH, HD), 1)
    q2 = jnp.where((row // BATCH) == (lane // HEAD_DIM), q2, 0.0)
    rb = row % BATCH
    return jnp.concatenate([jnp.where(rb == b, q2, 0.0).astype(BF16) for b in range(BATCH)], axis=1)


def gather_heads(mixed):
    col = lax.broadcasted_iota(jnp.int32, (HD, 2 * BATCH), 1) % BATCH
    acc = jnp.zeros((HD, 2 * BATCH), F32)
    for b in range(BATCH):
        acc = jnp.where(col == b, mixed[b * HD:(b + 1) * HD], acc)
    t = acc.T
    lane = lax.broadcasted_iota(jnp.int32, (BATCH, HD), 1)
    return jnp.where(lane < HEAD_DIM, t[:BATCH], t[BATCH:])


def core_kernel(emb_ref, pos_ref, posn_ref, in_bias_ref, out_bias_ref, b_fc1_ref, ln_ref, lnf_ref,
                sk_hbm, sv_hbm, ck_hbm, cv_hbm, wqkv_hbm, wcq_hbm, wout_hbm, wfc1_hbm, wfc2_hbm,
                h_out, k_out, v_out,
                sk, sv, ck, cv, wqkv, wcq, wout, wfc1, wfc2,
                emb_rs, part_send, part_rs, hbuf, x_ref,
                load_sems, rs_send, rs_recv, ag_send, ag_recv):
    me = lax.axis_index('tp')

    def load(src, dst, i):
        return pltpu.make_async_copy(src, dst, load_sems.at[i])

    loads = {}
    order = []
    for l in range(LAYERS):
        order += [('wqkv', l), ('sk', l), ('sv', l), ('wout', l), ('wcq', l), ('ck', l), ('cv', l), ('fc1', l), ('fc2', l)]
    refs = {'wqkv': (wqkv_hbm, wqkv), 'sk': (sk_hbm, sk), 'sv': (sv_hbm, sv), 'wout': (wout_hbm, wout),
            'wcq': (wcq_hbm, wcq), 'ck': (ck_hbm, ck), 'cv': (cv_hbm, cv), 'fc1': (wfc1_hbm, wfc1), 'fc2': (wfc2_hbm, wfc2)}
    single = ('sk', 'sv', 'ck', 'cv')
    for i, (name, l) in enumerate(order):
        src, dst = refs[name]
        loads[name, l] = load(src.at[l], dst if name in single else dst.at[l], i)
    for name, l in order:
        if l == 0 or name not in single:
            loads[name, l].start()

    barrier = pltpu.get_barrier_semaphore()
    for d in range(N_TP):
        @pl.when(me != d)
        def _():
            pl.semaphore_signal(barrier, inc=1, device_id={'tp': d}, device_id_type=MESH)
    pl.semaphore_wait(barrier, N_TP - 1)

    def rs_copy(ph, g, src, dst):
        return pltpu.make_async_remote_copy(src_ref=src, dst_ref=dst, send_sem=rs_send.at[ph, g], recv_sem=rs_recv.at[ph, me],
                                            device_id={'tp': OWNERS[g]}, device_id_type=MESH)

    def exchange(ph, src, rs_at, bias, gain, shift):
        for g in range(2):
            @pl.when(me != OWNERS[g])
            def _():
                rs_copy(ph, g, src(g), rs_at(me)).start()
        for g in range(2):
            owner = OWNERS[g]

            @pl.when(me == owner)
            def _():
                total = src(g)[...].astype(F32)
                for s in range(N_TP):
                    if s != owner:
                        pltpu.make_async_remote_copy(src_ref=src(g), dst_ref=rs_at(s), send_sem=rs_send.at[ph, g], recv_sem=rs_recv.at[ph, s],
                                                     device_id={'tp': owner}, device_id_type=MESH).wait_recv()
                        total = total + rs_at(s)[...].astype(F32)
                total = total.astype(BF16).astype(F32)
                x = total + pos_ref[g].astype(F32) if ph == 0 else x_ref[...] + total + bias
                if ph < N_PHASES - 1:
                    x_ref[...] = x
                hbuf[ph, g] = layer_norm(x, gain, shift)
                for d in range(N_TP):
                    if d != owner:
                        ag_copy(ph, g, d).start()
        for g in range(2):
            @pl.when(me != OWNERS[g])
            def _():
                ag_copy(ph, g, 0).wait_recv()
        return jnp.concatenate([hbuf[ph, 0], hbuf[ph, 1]], axis=0)

    def ag_copy(ph, g, d):
        return pltpu.make_async_remote_copy(src_ref=hbuf.at[ph, g], dst_ref=hbuf.at[ph, g], send_sem=ag_send.at[ph, d], recv_sem=ag_recv.at[ph, g],
                                            device_id={'tp': d}, device_id_type=MESH)

    def exchange_part(ph, part, bias, gain, shift):
        part_send[ph - 1, 0] = part[:ROWS]
        part_send[ph - 1, 1] = part[ROWS:]
        return exchange(ph, lambda g: part_send.at[ph - 1, g], lambda i: part_rs.at[ph - 1, i], bias, gain, shift)

    def ln_of(l, i):
        return ln_ref[l, i, 0:1], ln_ref[l, i, 1:2]

    hidden = exchange(0, lambda g: emb_ref.at[g], lambda i: emb_rs.at[i], None, *ln_of(0, 0))

    posn = posn_ref[...]
    t_idx = lax.broadcasted_iota(jnp.int32, (2 * BATCH, sk.shape[1]), 1)
    live = t_idx <= posn
    here = t_idx == posn
    qk_scale = HEAD_DIM ** -0.5

    for l in range(LAYERS):
        loads['wqkv', l].wait()
        qkv = dot_nt(hidden, wqkv[l])
        q = (qkv[:, :HD] + head_row(in_bias_ref, l, 0)).astype(BF16).astype(F32)
        k_new = qkv[:, HD:2 * HD].astype(BF16)
        v_new = (qkv[:, 2 * HD:] + head_row(in_bias_ref, l, 1)).astype(BF16)
        k_out[l] = k_new
        v_out[l] = v_new
        prod = q * k_new.astype(F32)
        s_new = jnp.concatenate([jnp.sum(prod[:, :HEAD_DIM], axis=1, keepdims=True), jnp.sum(prod[:, HEAD_DIM:], axis=1, keepdims=True)], axis=0)
        qs = spread_queries(q)
        loads['sk', l].wait()
        s = jnp.where(here, s_new, dot(qs, sk[...])) * qk_scale
        s = jnp.where(live, s, NEG)
        e = jnp.exp(s - jnp.max(s, axis=-1, keepdims=True))
        w = (e / jnp.sum(e, axis=-1, keepdims=True)).astype(BF16).astype(F32)
        w_new = jnp.sum(jnp.where(here, w, 0.0), axis=-1, keepdims=True)
        w_old = jnp.where(here, 0.0, w)
        loads['sv', l].wait()
        mixed = gather_heads(dot(sv[...], w_old.T.astype(BF16)))
        lane = lax.broadcasted_iota(jnp.int32, (BATCH, HD), 1)
        w_row = jnp.where(lane < HEAD_DIM, w_new[:BATCH], w_new[BATCH:])
        o = (mixed + w_row * v_new.astype(F32)).astype(BF16)
        if l + 1 < LAYERS:
            loads['sk', l + 1].start()
            loads['sv', l + 1].start()
        loads['wout', l].wait()
        hidden = exchange_part(3 * l + 1, dot(o, wout[l, 0]), out_bias_ref[0, l:l + 1], *ln_of(l, 1))

        loads['wcq', l].wait()
        q = (dot_nt(hidden, wcq[l]) + head_row(in_bias_ref, l, 2)).astype(BF16).astype(F32)
        qs = spread_queries(q)
        loads['ck', l].wait()
        s = dot(qs, ck[...]) * qk_scale
        e = jnp.exp(s - jnp.max(s, axis=-1, keepdims=True))
        w = e / jnp.sum(e, axis=-1, keepdims=True)
        loads['cv', l].wait()
        o = gather_heads(dot(cv[...], w.T.astype(BF16))).astype(BF16)
        if l + 1 < LAYERS:
            loads['ck', l + 1].start()
            loads['cv', l + 1].start()
        hidden = exchange_part(3 * l + 2, dot(o, wout[l, 1]), out_bias_ref[1, l:l + 1], *ln_of(l, 2))

        loads['fc1', l].wait()
        f = dot(hidden, wfc1[l]) + b_fc1_ref[l:l + 1]
        act = (f * 0.5 * (1.0 + lax.erf(f * (2.0 ** -0.5)))).astype(BF16)
        loads['fc2', l].wait()
        part = dot(act, wfc2[l])
        nxt = ln_of(l + 1, 0) if l + 1 < LAYERS else (lnf_ref[0:1], lnf_ref[1:2])
        hidden = exchange_part(3 * l + 3, part, out_bias_ref[2, l:l + 1], *nxt)

    h_out[...] = hidden

    for ph in range(N_PHASES):
        for g in range(2):
            src = emb_ref.at[g] if ph == 0 else part_send.at[ph - 1, g]
            dst = emb_rs.at[me] if ph == 0 else part_rs.at[ph - 1, me]

            @pl.when(me != OWNERS[g])
            def _():
                rs_copy(ph, g, src, dst).wait_send()

            @pl.when(me == OWNERS[g])
            def _():
                for d in range(N_TP):
                    if d != OWNERS[g]:
                        ag_copy(ph, g, d).wait_send()


def run_core(emb, pos, posn, in_bias, out_bias, b_fc1, ln_layers, ln_final, sk, sv, ck, cv, wqkv, wcq, wout, wfc1, wfc2):
    vm = pl.BlockSpec(memory_space=pltpu.VMEM)
    hbm = pl.BlockSpec(memory_space=pl.ANY)
    d_model = emb.shape[-1]
    per_layer = [sk, sv, ck, cv]
    n_loads = 9 * LAYERS
    return pl.pallas_call(
        core_kernel,
        out_shape=(jax.ShapeDtypeStruct((BATCH, d_model), BF16),
                   jax.ShapeDtypeStruct((LAYERS, BATCH, HD), BF16), jax.ShapeDtypeStruct((LAYERS, BATCH, HD), BF16)),
        in_specs=[vm] * 8 + [hbm] * 9,
        out_specs=(vm, vm, vm),
        scratch_shapes=[pltpu.VMEM(a.shape[1:], BF16) for a in per_layer]
        + [pltpu.VMEM(a.shape, BF16) for a in (wqkv, wcq, wout, wfc1, wfc2)]
        + [pltpu.VMEM((N_TP, ROWS, d_model), BF16),
           pltpu.VMEM((N_PHASES - 1, 2, ROWS, d_model), F32),
           pltpu.VMEM((N_PHASES - 1, N_TP, ROWS, d_model), F32),
           pltpu.VMEM((N_PHASES, 2, ROWS, d_model), BF16),
           pltpu.VMEM((ROWS, d_model), F32),
           pltpu.SemaphoreType.DMA((n_loads,)),
           pltpu.SemaphoreType.DMA((N_PHASES, 2)),
           pltpu.SemaphoreType.DMA((N_PHASES, N_TP)),
           pltpu.SemaphoreType.DMA((N_PHASES, N_TP)),
           pltpu.SemaphoreType.DMA((N_PHASES, 2))],
        compiler_params=pltpu.CompilerParams(collective_id=0, has_side_effects=True, vmem_limit_bytes=40 << 20),
        name='decode_layers',
    )(emb, pos, posn, in_bias, out_bias, b_fc1, ln_layers, ln_final, sk, sv, ck, cv, wqkv, wcq, wout, wfc1, wfc2)


def solution(mesh):
    def local_step(tokens, positions, self_keys, self_vals, cross_keys, cross_vals, embed_table, pos_table, w_qkv, w_cq, in_bias, w_out, out_bias, w_fc1, b_fc1, w_fc2, ln_layers, ln_final):
        shard_rows, d_model = embed_table.shape
        local_ids = tokens - lax.axis_index('tp') * shard_rows
        owned = (local_ids >= 0) & (local_ids < shard_rows)
        picked = jnp.take(embed_table, jnp.clip(local_ids, 0, shard_rows - 1), axis=0)
        picked = jnp.where(owned[:, None], picked, jnp.zeros_like(picked)).reshape(2, ROWS, d_model)
        pos_rows = jnp.take(pos_table, positions, axis=0).reshape(2, ROWS, d_model)
        posn = jnp.concatenate([positions, positions])[:, None]

        def rows_by_time(cache):
            return jnp.transpose(cache, (0, 1, 3, 4, 2)).reshape(LAYERS, BATCH * HD, cache.shape[2])

        hidden, k_new, v_new = run_core(
            picked, pos_rows, posn, in_bias, jnp.transpose(out_bias, (1, 0, 2)), b_fc1, ln_layers, ln_final,
            rows_by_time(self_keys), rows_by_time(self_vals), rows_by_time(cross_keys), rows_by_time(cross_vals),
            jnp.transpose(w_qkv, (0, 2, 3, 4, 1)).reshape(LAYERS, 3 * HD, d_model),
            jnp.transpose(w_cq, (0, 2, 3, 1)).reshape(LAYERS, HD, d_model),
            w_out.reshape(LAYERS, 2, HD, d_model), w_fc1, w_fc2)
        logits = jnp.einsum('bd,vd->bv', hidden, embed_table, preferred_element_type=F32)
        cache_pos = jnp.arange(self_keys.shape[2])[None, :]
        write_mask = (cache_pos == positions[:, None])[None, :, :, None, None]
        shape = (LAYERS, BATCH, 1, HEADS, HEAD_DIM)
        new_keys = jnp.where(write_mask, k_new.reshape(shape), self_keys)
        new_vals = jnp.where(write_mask, v_new.reshape(shape), self_vals)
        return logits, new_keys, new_vals

    batch_spec = P('dp')
    cache_spec = P(None, 'dp', None, 'tp', None)
    in_specs = (batch_spec, batch_spec, cache_spec, cache_spec, cache_spec, cache_spec, P('tp', None), P(None, None), P(None, None, None, 'tp', None), P(None, None, 'tp', None), P(None, None, 'tp', None), P(None, None, 'tp', None, None), P(None, None, None), P(None, None, 'tp'), P(None, 'tp'), P(None, 'tp', None), P(None, None, None, None), P(None, None))
    out_specs = (P('dp', 'tp'), cache_spec, cache_spec)
    return jax.shard_map(local_step, mesh=mesh, in_specs=in_specs, out_specs=out_specs, check_vma=False)
```

```python
import functools

import jax
import jax.numpy as jnp
from jax import lax
from jax.experimental import pallas as pl
from jax.experimental.pallas import tpu as pltpu
from jax.sharding import PartitionSpec as P

BF16 = jnp.bfloat16
F32 = jnp.float32
MESH = pl.DeviceIdType.MESH
N_TP = 8
OWNERS = (3, 5)
ROWS = 8
BATCH = 16
HEADS = 2
HEAD_DIM = 64
HD = HEADS * HEAD_DIM
LAYERS = 2
N_PHASES = 1 + 3 * LAYERS
CORE_VMEM = 30 << 20
GATHER_VMEM = 4 << 20
FINAL_VMEM = 6 << 20
NEG = -1e30


def dot(a, b):
    return jnp.dot(a, b, preferred_element_type=F32)


def dot_nt(a, b):
    return lax.dot_general(a, b, (((1,), (1,)), ((), ())), preferred_element_type=F32)


def in_hbm(*arrays):
    return tuple(pltpu.with_memory_space_constraint(a, pltpu.HBM) for a in arrays)


def layer_norm(x, gain, shift):
    mean = jnp.mean(x, axis=-1, keepdims=True)
    centred = x - mean
    var = jnp.mean(centred * centred, axis=-1, keepdims=True)
    return (centred * lax.rsqrt(var + 1e-5) * gain + shift).astype(BF16)


def head_row(ref, *idx):
    v = ref[idx]
    return jnp.concatenate([v[0:1], v[1:2]], axis=1)


def spread_queries(q):
    q2 = jnp.concatenate([q, q], axis=0)
    row = lax.broadcasted_iota(jnp.int32, (2 * BATCH, HD), 0)
    lane = lax.broadcasted_iota(jnp.int32, (2 * BATCH, HD), 1)
    q2 = jnp.where((row // BATCH) == (lane // HEAD_DIM), q2, 0.0)
    rb = row % BATCH
    return jnp.concatenate([jnp.where(rb == b, q2, 0.0).astype(BF16) for b in range(BATCH)], axis=1)


def gather_heads(mixed):
    col = lax.broadcasted_iota(jnp.int32, (HD, 2 * BATCH), 1) % BATCH
    acc = jnp.zeros((HD, 2 * BATCH), F32)
    for b in range(BATCH):
        acc = jnp.where(col == b, mixed[b * HD:(b + 1) * HD], acc)
    t = acc.T
    lane = lax.broadcasted_iota(jnp.int32, (BATCH, HD), 1)
    return jnp.where(lane < HEAD_DIM, t[:BATCH], t[BATCH:])


def core_kernel(emb_ref, pos_ref, posn_ref, in_bias_hbm, out_bias_hbm, b_fc1_hbm, ln_hbm, lnf_hbm,
                table_hbm, sk_hbm, sv_hbm, ck_hbm, cv_hbm, wqkv_hbm, wcq_hbm, wout_hbm, wfc1_hbm, wfc2_hbm,
                h_out, table, sk, sv,
                ck, cv, wqkv, wcq, wout, wfc1, wfc2,
                in_bias_ref, out_bias_ref, b_fc1_ref, ln_ref, lnf_ref,
                emb_rs, part_send, part_rs, hbuf, x_ref,
                load_sems, rs_send, rs_recv, ag_send, ag_recv):
    me = lax.axis_index('tp')

    def load(src, dst, i):
        return pltpu.make_async_copy(src, dst, load_sems.at[i])

    smalls = [(in_bias_hbm, in_bias_ref), (out_bias_hbm, out_bias_ref), (b_fc1_hbm, b_fc1_ref), (ln_hbm, ln_ref), (lnf_hbm, lnf_ref)]
    small_loads = [load(src, dst, 9 * LAYERS + i) for i, (src, dst) in enumerate(smalls)]
    for c in small_loads:
        c.start()
    loads = {}
    order = []
    for l in range(LAYERS):
        order += [('wqkv', l), ('sk', l), ('sv', l), ('wout', l), ('wcq', l), ('ck', l), ('cv', l), ('fc1', l), ('fc2', l)]
    refs = {'wqkv': (wqkv_hbm, wqkv), 'sk': (sk_hbm, sk), 'sv': (sv_hbm, sv), 'wout': (wout_hbm, wout),
            'wcq': (wcq_hbm, wcq), 'ck': (ck_hbm, ck), 'cv': (cv_hbm, cv), 'fc1': (wfc1_hbm, wfc1), 'fc2': (wfc2_hbm, wfc2)}
    single = ('ck', 'cv')
    for i, (name, l) in enumerate(order):
        src, dst = refs[name]
        loads[name, l] = load(src.at[l], dst if name in single else dst.at[l], i)
    for name, l in order:
        if l == 0 or name not in single:
            loads[name, l].start()
    table_load = load(table_hbm, table, len(order) + len(smalls))
    table_load.start()

    barrier = pltpu.get_barrier_semaphore()
    for d in range(N_TP):
        @pl.when(me != d)
        def _():
            pl.semaphore_signal(barrier, inc=1, device_id={'tp': d}, device_id_type=MESH)
    pl.semaphore_wait(barrier, N_TP - 1)

    def rs_copy(ph, g, src, dst):
        return pltpu.make_async_remote_copy(src_ref=src, dst_ref=dst, send_sem=rs_send.at[ph, g], recv_sem=rs_recv.at[ph, me],
                                            device_id={'tp': OWNERS[g]}, device_id_type=MESH)

    def exchange(ph, src, rs_at, bias, gain, shift, meanwhile=None):
        for g in range(2):
            @pl.when(me != OWNERS[g])
            def _():
                rs_copy(ph, g, src(g), rs_at(me)).start()
        if meanwhile is not None:
            meanwhile()
        for g in range(2):
            owner = OWNERS[g]

            @pl.when(me == owner)
            def _():
                total = src(g)[...].astype(F32)
                for s in range(N_TP):
                    if s != owner:
                        pltpu.make_async_remote_copy(src_ref=src(g), dst_ref=rs_at(s), send_sem=rs_send.at[ph, g], recv_sem=rs_recv.at[ph, s],
                                                     device_id={'tp': owner}, device_id_type=MESH).wait_recv()
                        total = total + rs_at(s)[...].astype(F32)
                total = total.astype(BF16).astype(F32)
                x = total + pos_ref[g].astype(F32) if ph == 0 else x_ref[...] + total + bias
                if ph < N_PHASES - 1:
                    x_ref[...] = x
                hbuf[ph, g] = layer_norm(x, gain, shift)
                for d in range(N_TP):
                    if d != owner:
                        ag_copy(ph, g, d).start()
        for g in range(2):
            @pl.when(me != OWNERS[g])
            def _():
                ag_copy(ph, g, 0).wait_recv()
        return jnp.concatenate([hbuf[ph, 0], hbuf[ph, 1]], axis=0)

    def ag_copy(ph, g, d):
        return pltpu.make_async_remote_copy(src_ref=hbuf.at[ph, g], dst_ref=hbuf.at[ph, g], send_sem=ag_send.at[ph, d], recv_sem=ag_recv.at[ph, g],
                                            device_id={'tp': d}, device_id_type=MESH)

    def exchange_part(ph, part, bias, gain, shift, meanwhile=None):
        part_send[ph - 1, 0] = part[:ROWS]
        part_send[ph - 1, 1] = part[ROWS:]
        return exchange(ph, lambda g: part_send.at[ph - 1, g], lambda i: part_rs.at[ph - 1, i], bias, gain, shift, meanwhile)

    for c in small_loads:
        c.wait()

    def ln_of(l, i):
        return ln_ref[l, i, 0:1], ln_ref[l, i, 1:2]

    hidden = exchange(0, lambda g: emb_ref.at[g], lambda i: emb_rs.at[i], None, *ln_of(0, 0))

    time = sk.shape[2]

    def masks():
        t_idx = lax.broadcasted_iota(jnp.int32, (2 * BATCH, time), 1)
        posn = posn_ref[...]
        return t_idx <= posn, t_idx == posn
    qk_scale = HEAD_DIM ** -0.5

    for l in range(LAYERS):
        loads['wqkv', l].wait()
        qkv = dot_nt(hidden, wqkv[l])
        q = (qkv[:, :HD] + head_row(in_bias_ref, l, 0)).astype(BF16).astype(F32)
        k_new = qkv[:, HD:2 * HD].astype(BF16)
        v_new = (qkv[:, 2 * HD:] + head_row(in_bias_ref, l, 1)).astype(BF16)
        live, here = masks()
        prod = q * k_new.astype(F32)
        s_new = jnp.concatenate([jnp.sum(prod[:, :HEAD_DIM], axis=1, keepdims=True), jnp.sum(prod[:, HEAD_DIM:], axis=1, keepdims=True)], axis=0)
        qs = spread_queries(q)
        loads['sk', l].wait()
        s = jnp.where(here, s_new, dot(qs, sk[l])) * qk_scale
        s = jnp.where(live, s, NEG)
        e = jnp.exp(s - jnp.max(s, axis=-1, keepdims=True))
        w = (e / jnp.sum(e, axis=-1, keepdims=True)).astype(BF16).astype(F32)
        w_new = jnp.sum(jnp.where(here, w, 0.0), axis=-1, keepdims=True)
        w_old = jnp.where(here, 0.0, w)
        loads['sv', l].wait()
        mixed = gather_heads(dot(sv[l], w_old.T.astype(BF16)))
        lane = lax.broadcasted_iota(jnp.int32, (BATCH, HD), 1)
        w_row = jnp.where(lane < HEAD_DIM, w_new[:BATCH], w_new[BATCH:])
        o = (mixed + w_row * v_new.astype(F32)).astype(BF16)

        def write_new():
            t_row = lax.broadcasted_iota(jnp.int32, (HD, time), 1)
            k_cols, v_cols = k_new.astype(F32).T, v_new.astype(F32).T
            for b in range(BATCH):
                at = t_row == posn_ref[b:b + 1]
                rows = pl.ds(b * HD, HD)
                sk[l, rows] = jnp.where(at, k_cols[:, b:b + 1], sk[l, rows].astype(F32)).astype(BF16)
                sv[l, rows] = jnp.where(at, v_cols[:, b:b + 1], sv[l, rows].astype(F32)).astype(BF16)

        loads['wout', l].wait()
        hidden = exchange_part(3 * l + 1, dot(o, wout[l, 0]), out_bias_ref[0, l:l + 1], *ln_of(l, 1), write_new)

        loads['wcq', l].wait()
        q = (dot_nt(hidden, wcq[l]) + head_row(in_bias_ref, l, 2)).astype(BF16).astype(F32)
        qs = spread_queries(q)
        loads['ck', l].wait()
        s = dot(qs, ck[...]) * qk_scale
        e = jnp.exp(s - jnp.max(s, axis=-1, keepdims=True))
        w = e / jnp.sum(e, axis=-1, keepdims=True)
        loads['cv', l].wait()
        o = gather_heads(dot(cv[...], w.T.astype(BF16))).astype(BF16)
        if l + 1 < LAYERS:
            loads['ck', l + 1].start()
            loads['cv', l + 1].start()
        hidden = exchange_part(3 * l + 2, dot(o, wout[l, 1]), out_bias_ref[1, l:l + 1], *ln_of(l, 2))

        loads['fc1', l].wait()
        f = dot(hidden, wfc1[l]) + b_fc1_ref[l:l + 1]
        act = (f * 0.5 * (1.0 + lax.erf(f * (2.0 ** -0.5)))).astype(BF16)
        loads['fc2', l].wait()
        part = dot(act, wfc2[l])
        nxt = ln_of(l + 1, 0) if l + 1 < LAYERS else (lnf_ref[0:1], lnf_ref[1:2])
        hidden = exchange_part(3 * l + 3, part, out_bias_ref[2, l:l + 1], *nxt)

    h_out[...] = hidden
    table_load.wait()

    for ph in range(N_PHASES):
        for g in range(2):
            src = emb_ref.at[g] if ph == 0 else part_send.at[ph - 1, g]
            dst = emb_rs.at[me] if ph == 0 else part_rs.at[ph - 1, me]

            @pl.when(me != OWNERS[g])
            def _():
                rs_copy(ph, g, src, dst).wait_send()

            @pl.when(me == OWNERS[g])
            def _():
                for d in range(N_TP):
                    if d != OWNERS[g]:
                        ag_copy(ph, g, d).wait_send()


def run_core(emb, pos, posn, in_bias, out_bias, b_fc1, ln_layers, ln_final, table, sk, sv, ck, cv, wqkv, wcq, wout, wfc1, wfc2):
    vm = pl.BlockSpec(memory_space=pltpu.VMEM)
    hbm = pl.BlockSpec(memory_space=pltpu.HBM)
    d_model = emb.shape[-1]
    smalls = (in_bias, out_bias, b_fc1, ln_layers, ln_final)
    n_loads = 9 * LAYERS + len(smalls) + 1
    return pl.pallas_call(
        core_kernel,
        out_shape=(pltpu.VMEM((BATCH, d_model), BF16),) + tuple(pltpu.VMEM(a.shape, BF16) for a in (table, sk, sv)),
        in_specs=[vm] * 3 + [hbm] * 15,
        out_specs=(vm,) * 4,
        scratch_shapes=[pltpu.VMEM(a.shape[1:], BF16) for a in (ck, cv)]
        + [pltpu.VMEM(a.shape, BF16) for a in (wqkv, wcq, wout, wfc1, wfc2)]
        + [pltpu.VMEM(a.shape, F32) for a in smalls]
        + [pltpu.VMEM((N_TP, ROWS, d_model), BF16),
           pltpu.VMEM((N_PHASES - 1, 2, ROWS, d_model), F32),
           pltpu.VMEM((N_PHASES - 1, N_TP, ROWS, d_model), F32),
           pltpu.VMEM((N_PHASES, 2, ROWS, d_model), BF16),
           pltpu.VMEM((ROWS, d_model), F32),
           pltpu.SemaphoreType.DMA((n_loads,)),
           pltpu.SemaphoreType.DMA((N_PHASES, 2)),
           pltpu.SemaphoreType.DMA((N_PHASES, N_TP)),
           pltpu.SemaphoreType.DMA((N_PHASES, N_TP)),
           pltpu.SemaphoreType.DMA((N_PHASES, 2))],
        compiler_params=pltpu.CompilerParams(collective_id=0, has_side_effects=True, vmem_limit_bytes=CORE_VMEM),
        cost_estimate=pl.CostEstimate(flops=4 << 30, bytes_accessed=150 << 20, transcendentals=0),
        name='decode_layers',
    )(emb, pos, posn, *in_hbm(in_bias, out_bias, b_fc1, ln_layers, ln_final, table, sk, sv, ck, cv, wqkv, wcq, wout, wfc1, wfc2))


def gather_kernel(tok_hbm, posn_hbm, table_hbm, pos_hbm, emb_out, pos_out, posn_out, emb_buf, pos_buf, tok_ref, pos_ref, sems, idx_sems):
    idx = [pltpu.make_async_copy(tok_hbm, tok_ref, idx_sems.at[0]), pltpu.make_async_copy(posn_hbm, pos_ref, idx_sems.at[1])]
    for c in idx:
        c.start()
    for c in idx:
        c.wait()
    shard_rows = table_hbm.shape[0]
    base = lax.axis_index('tp') * shard_rows
    copies = []
    for b in range(BATCH):
        row = jnp.clip(tok_ref[b] - base, 0, shard_rows - 1)
        at = pl.multiple_of((row // 8) * 8, 8)
        copies.append(pltpu.make_async_copy(table_hbm.at[pl.ds(at, 8)], emb_buf.at[pl.ds(b * 8, 8)], sems.at[0, b]))
        at = pl.multiple_of((pos_ref[b] // 8) * 8, 8)
        copies.append(pltpu.make_async_copy(pos_hbm.at[pl.ds(at, 8)], pos_buf.at[pl.ds(b * 8, 8)], sems.at[1, b]))
    for c in copies:
        c.start()
    row_i = lax.broadcasted_iota(jnp.int32, (BATCH, 8 * BATCH), 0)
    lane_i = lax.broadcasted_iota(jnp.int32, (BATCH, 8 * BATCH), 1)
    tok_at = jnp.zeros((BATCH, 8 * BATCH), jnp.int32)
    pos_at = jnp.zeros((BATCH, 8 * BATCH), jnp.int32)
    posn_row = lax.broadcasted_iota(jnp.int32, (BATCH, posn_out.shape[1]), 0)
    posn = jnp.zeros(posn_row.shape, jnp.int32)
    for b in range(BATCH):
        row = tok_ref[b] - base
        owned = (row >= 0) & (row < shard_rows)
        tok_at = jnp.where(row_i == b, jnp.where(owned, b * 8 + row % 8, -1), tok_at)
        pos_at = jnp.where(row_i == b, b * 8 + pos_ref[b] % 8, pos_at)
        posn = jnp.where(posn_row == b, pos_ref[b], posn)
    posn_out[...] = jnp.concatenate([posn, posn], axis=0)
    pick_tok = jnp.where(lane_i == tok_at, 1.0, 0.0).astype(BF16)
    pick_pos = jnp.where(lane_i == pos_at, 1.0, 0.0).astype(BF16)
    for c in copies:
        c.wait()
    emb = dot(pick_tok, emb_buf[...]).astype(BF16)
    pos = dot(pick_pos, pos_buf[...]).astype(BF16)
    for g in range(2):
        emb_out[g] = emb[g * ROWS:(g + 1) * ROWS]
        pos_out[g] = pos[g * ROWS:(g + 1) * ROWS]


def run_gather(tokens, positions, embed_table, pos_table, time):
    vm = pl.BlockSpec(memory_space=pltpu.VMEM)
    hbm = pl.BlockSpec(memory_space=pltpu.HBM)
    d_model = embed_table.shape[1]
    rows = pltpu.VMEM((2, ROWS, d_model), BF16)
    return pl.pallas_call(
        gather_kernel,
        out_shape=(rows, rows, pltpu.VMEM((2 * BATCH, time), jnp.int32)),
        in_specs=[hbm] * 4,
        out_specs=(vm, vm, vm),
        scratch_shapes=[pltpu.VMEM((8 * BATCH, d_model), BF16), pltpu.VMEM((8 * BATCH, d_model), BF16),
                        pltpu.SMEM((BATCH,), jnp.int32), pltpu.SMEM((BATCH,), jnp.int32),
                        pltpu.SemaphoreType.DMA((2, BATCH)), pltpu.SemaphoreType.DMA((2,))],
        compiler_params=pltpu.CompilerParams(vmem_limit_bytes=GATHER_VMEM),
        name='gather_rows',
    )(*in_hbm(tokens, positions, embed_table, pos_table))


N_TILES = 3


def final_kernel(h_ref, table_ref, sk_ref, sv_ref, logits_ref, sk_out, sv_out, sems):
    copies = [pltpu.make_async_copy(sk_ref, sk_out, sems.at[0]), pltpu.make_async_copy(sv_ref, sv_out, sems.at[1])]
    for c in copies:
        c.start()
    h_t = h_ref[...].astype(F32).T.astype(BF16)
    tile = table_ref.shape[0] // N_TILES
    for i in range(N_TILES):
        logits_ref[:, i * tile:(i + 1) * tile] = dot(table_ref[i * tile:(i + 1) * tile], h_t).T
    for c in copies:
        c.wait()


def run_final(hidden, table, sk, sv):
    vm = pl.BlockSpec(memory_space=pltpu.VMEM)
    hbm = pl.BlockSpec(memory_space=pltpu.HBM)
    cache = jax.ShapeDtypeStruct(sk.shape, BF16)
    return pl.pallas_call(
        final_kernel,
        out_shape=(jax.ShapeDtypeStruct((BATCH, table.shape[0]), F32), cache, cache),
        in_specs=[vm] * 4,
        out_specs=(vm, hbm, hbm),
        scratch_shapes=[pltpu.SemaphoreType.DMA((2,))],
        compiler_params=pltpu.CompilerParams(vmem_limit_bytes=FINAL_VMEM),
        name='logits_and_caches',
    )(hidden, table, sk, sv)


def solution(mesh):
    def local_step(tokens, positions, self_keys, self_vals, cross_keys, cross_vals, embed_table, pos_table, w_qkv, w_cq, in_bias, w_out, out_bias, w_fc1, b_fc1, w_fc2, ln_layers, ln_final):
        d_model = embed_table.shape[1]

        def rows_by_time(cache):
            return jnp.transpose(cache, (0, 1, 3, 4, 2)).reshape(LAYERS, BATCH * HD, cache.shape[2])

        def as_cache(rows):
            return jnp.transpose(rows.reshape(LAYERS, BATCH, HEADS, HEAD_DIM, rows.shape[2]), (0, 1, 4, 2, 3))

        sk, sv = rows_by_time(self_keys), rows_by_time(self_vals)
        emb, pos, posn = run_gather(tokens, positions, embed_table, pos_table, sk.shape[2])
        hidden, table, sk, sv = run_core(
            emb, pos, posn, in_bias, jnp.transpose(out_bias, (1, 0, 2)), b_fc1, ln_layers, ln_final,
            embed_table, sk, sv, rows_by_time(cross_keys), rows_by_time(cross_vals),
            jnp.transpose(w_qkv, (0, 2, 3, 4, 1)).reshape(LAYERS, 3 * HD, d_model),
            jnp.transpose(w_cq, (0, 2, 3, 1)).reshape(LAYERS, HD, d_model),
            w_out.reshape(LAYERS, 2, HD, d_model), w_fc1, w_fc2)
        logits, new_sk, new_sv = run_final(hidden, table, sk, sv)
        return logits, as_cache(new_sk), as_cache(new_sv)

    batch_spec = P('dp')
    cache_spec = P(None, 'dp', None, 'tp', None)
    in_specs = (batch_spec, batch_spec, cache_spec, cache_spec, cache_spec, cache_spec, P('tp', None), P(None, None), P(None, None, None, 'tp', None), P(None, None, 'tp', None), P(None, None, 'tp', None), P(None, None, 'tp', None, None), P(None, None, None), P(None, None, 'tp'), P(None, 'tp'), P(None, 'tp', None), P(None, None, None, None), P(None, None))
    out_specs = (P('dp', 'tp'), cache_spec, cache_spec)
    return jax.shard_map(local_step, mesh=mesh, in_specs=in_specs, out_specs=out_specs, check_vma=False)
```

```python
import functools

import jax
import jax.numpy as jnp
from jax import lax
from jax.experimental import pallas as pl
from jax.experimental.pallas import tpu as pltpu
from jax.sharding import PartitionSpec as P

BF16 = jnp.bfloat16
F32 = jnp.float32
MESH = pl.DeviceIdType.MESH
N_TP = 8
OWNERS = (3, 5)
NEAR_FIRST = ((2, 1, 0, 5, 4, 7, 6), (4, 7, 6, 3, 2, 1, 0))
ROWS = 8
BATCH = 16
HEADS = 2
HEAD_DIM = 64
HD = HEADS * HEAD_DIM
LAYERS = 2
GROUP_ROWS = 8 * 128
N_PHASES = 1 + 3 * LAYERS
CORE_VMEM = 30 << 20
GATHER_VMEM = 4 << 20
FINAL_VMEM = 6 << 20
NEG = -1e30


def dot(a, b):
    return jnp.dot(a, b, preferred_element_type=F32)


def dot_nt(a, b):
    return lax.dot_general(a, b, (((1,), (1,)), ((), ())), preferred_element_type=F32)


def in_hbm(*arrays):
    return tuple(pltpu.with_memory_space_constraint(a, pltpu.HBM) for a in arrays)


def layer_norm(x, gain, shift):
    mean = jnp.mean(x, axis=-1, keepdims=True)
    centred = x - mean
    var = jnp.mean(centred * centred, axis=-1, keepdims=True)
    return (centred * lax.rsqrt(var + 1e-5) * gain + shift).astype(BF16)


def head_row(ref, *idx):
    v = ref[idx]
    return jnp.concatenate([v[0:1], v[1:2]], axis=1)


def spread_queries(q):
    q2 = jnp.concatenate([q, q], axis=0)
    row = lax.broadcasted_iota(jnp.int32, q2.shape, 0)
    lane = lax.broadcasted_iota(jnp.int32, q2.shape, 1)
    q2 = jnp.where((row // ROWS) == (lane // HEAD_DIM), q2, 0.0)
    rb = row % ROWS
    return jnp.concatenate([jnp.where(rb == b, q2, 0.0).astype(BF16) for b in range(ROWS)], axis=1)


def gather_heads(mixed):
    col = lax.broadcasted_iota(jnp.int32, (HD, HEADS * ROWS), 1) % ROWS
    acc = jnp.zeros(col.shape, F32)
    for b in range(ROWS):
        acc = jnp.where(col == b, mixed[b * HD:(b + 1) * HD], acc)
    t = acc.T
    lane = lax.broadcasted_iota(jnp.int32, (ROWS, HD), 1)
    return jnp.where(lane < HEAD_DIM, t[:ROWS], t[ROWS:])


def core_kernel(emb_ref, pos_ref, posn_ref, in_bias_hbm, out_bias_hbm, b_fc1_hbm, ln_hbm, lnf_hbm,
                table_hbm, sk_hbm, sv_hbm, ck_hbm, cv_hbm, wqkv_hbm, wcq_hbm, wout_hbm, wfc1_hbm, wfc2_hbm,
                h_out, table, sk, sv,
                ck, cv, wqkv, wcq, wout, wfc1, wfc2,
                in_bias_ref, out_bias_ref, b_fc1_ref, ln_ref, lnf_ref,
                emb_rs, part_send, part_rs, hbuf, x_ref,
                load_sems, rs_send, rs_recv, ag_send, ag_recv):
    me = lax.axis_index('tp')

    def load(src, dst, i):
        return pltpu.make_async_copy(src, dst, load_sems.at[i])

    smalls = [(in_bias_hbm, in_bias_ref), (out_bias_hbm, out_bias_ref), (b_fc1_hbm, b_fc1_ref), (ln_hbm, ln_ref), (lnf_hbm, lnf_ref)]
    small_loads = [load(src, dst, i) for i, (src, dst) in enumerate(smalls)]
    for c in small_loads:
        c.start()
    refs = {'wqkv': (wqkv_hbm, wqkv), 'sk': (sk_hbm, sk), 'sv': (sv_hbm, sv), 'wout': (wout_hbm, wout),
            'wcq': (wcq_hbm, wcq), 'ck': (ck_hbm, ck), 'cv': (cv_hbm, cv), 'fc1': (wfc1_hbm, wfc1), 'fc2': (wfc2_hbm, wfc2)}
    half = GROUP_ROWS
    loads = {}
    for l in range(LAYERS):
        for name, (src, dst) in refs.items():
            for g in range(2):
                i = len(smalls) + len(loads)
                if name in ('ck', 'cv'):
                    loads[name, l, g] = load(src.at[l, pl.ds(g * half, half)], dst.at[pl.ds(g * half, half)], i)
                elif g == 0:
                    loads[name, l] = load(src.at[l], dst.at[l], i)
    table_load = load(table_hbm, table, len(smalls) + len(loads))
    for key, c in loads.items():
        if key[1] == 0:
            c.start()

    barrier = pltpu.get_barrier_semaphore()
    is_owner = (me == OWNERS[0]) | (me == OWNERS[1])
    for d in range(N_TP):
        @pl.when((me != d) if d in OWNERS else is_owner)
        def _():
            pl.semaphore_signal(barrier, inc=1, device_id={'tp': d}, device_id_type=MESH)

    @pl.when(is_owner)
    def _():
        pl.semaphore_wait(barrier, N_TP - 1)

    @pl.when(jnp.logical_not(is_owner))
    def _():
        pl.semaphore_wait(barrier, 2)

    def part_of(ph, g):
        return emb_ref.at[g] if ph == 0 else part_send.at[ph - 1, g]

    def landing(ph, i):
        return emb_rs.at[i] if ph == 0 else part_rs.at[ph - 1, i]

    def rs_copy(ph, g, i):
        return pltpu.make_async_remote_copy(src_ref=part_of(ph, g), dst_ref=landing(ph, i), send_sem=rs_send.at[ph, g], recv_sem=rs_recv.at[ph, i],
                                            device_id={'tp': OWNERS[g]}, device_id_type=MESH)

    def ag_copy(ph, g, d):
        return pltpu.make_async_remote_copy(src_ref=hbuf.at[ph, g], dst_ref=hbuf.at[ph, g], send_sem=ag_send.at[ph, d], recv_sem=ag_recv.at[ph, g],
                                            device_id={'tp': d}, device_id_type=MESH)

    def send(ph, g):
        @pl.when(me != OWNERS[g])
        def _():
            rs_copy(ph, g, me).start()

    def reduce(ph, g, bias, gain, shift):
        owner = OWNERS[g]

        @pl.when(me == owner)
        def _():
            total = part_of(ph, g)[...].astype(F32)
            for i in NEAR_FIRST[g]:
                rs_copy(ph, g, i).wait_recv()
                total = total + landing(ph, i)[...].astype(F32)
            total = total.astype(BF16).astype(F32)
            x = total + pos_ref[g].astype(F32) if ph == 0 else x_ref[...] + total + bias
            if ph < N_PHASES - 1:
                x_ref[...] = x
            hbuf[ph, g] = layer_norm(x, gain, shift)
            for d in reversed(NEAR_FIRST[g]):
                ag_copy(ph, g, d).start()

    def receive(ph, g):
        @pl.when(me != OWNERS[g])
        def _():
            ag_copy(ph, g, 0).wait_recv()
        return hbuf[ph, g]

    for g in range(2):
        send(0, g)
    for c in small_loads:
        c.wait()

    def ln_of(l, i):
        return ln_ref[l, i, 0:1], ln_ref[l, i, 1:2]

    for g in range(2):
        reduce(0, g, None, *ln_of(0, 0))

    time = sk.shape[2]
    qk_scale = HEAD_DIM ** -0.5

    def attend_self(l, g, hidden):
        qkv = dot_nt(hidden, wqkv[l])
        q = (qkv[:, :HD] + head_row(in_bias_ref, l, 0)).astype(BF16).astype(F32)
        k_new = qkv[:, HD:2 * HD].astype(BF16)
        v_new = (qkv[:, 2 * HD:] + head_row(in_bias_ref, l, 1)).astype(BF16)
        prod = q * k_new.astype(F32)
        s_new = jnp.concatenate([jnp.sum(prod[:, :HEAD_DIM], axis=1, keepdims=True), jnp.sum(prod[:, HEAD_DIM:], axis=1, keepdims=True)], axis=0)
        posn = posn_ref[g]
        t_idx = lax.broadcasted_iota(jnp.int32, posn.shape, 1)
        here = t_idx == posn
        rows = slice(g * half, (g + 1) * half)
        s = jnp.where(here, s_new, dot(spread_queries(q), sk[l, rows])) * qk_scale
        s = jnp.where(t_idx <= posn, s, NEG)
        e = jnp.exp(s - jnp.max(s, axis=-1, keepdims=True))
        w = (e / jnp.sum(e, axis=-1, keepdims=True)).astype(BF16).astype(F32)
        w_new = jnp.sum(jnp.where(here, w, 0.0), axis=-1, keepdims=True)
        w_old = jnp.where(here, 0.0, w)
        mixed = gather_heads(dot(sv[l, rows], w_old.T.astype(BF16)))
        lane = lax.broadcasted_iota(jnp.int32, (ROWS, HD), 1)
        w_row = jnp.where(lane < HEAD_DIM, w_new[:ROWS], w_new[ROWS:])
        o = (mixed + w_row * v_new.astype(F32)).astype(BF16)
        return dot(o, wout[l, 0]), (k_new, v_new)

    def write_new(l, g, k_new, v_new):
        t_row = lax.broadcasted_iota(jnp.int32, (HD, time), 1)
        k_cols, v_cols = k_new.astype(F32).T, v_new.astype(F32).T
        for b in range(ROWS):
            at = t_row == posn_ref[g, b:b + 1]
            rows = pl.ds(g * half + b * HD, HD)
            sk[l, rows] = jnp.where(at, k_cols[:, b:b + 1], sk[l, rows].astype(F32)).astype(BF16)
            sv[l, rows] = jnp.where(at, v_cols[:, b:b + 1], sv[l, rows].astype(F32)).astype(BF16)

    def attend_cross(l, g, hidden):
        q = (dot_nt(hidden, wcq[l]) + head_row(in_bias_ref, l, 2)).astype(BF16).astype(F32)
        rows = slice(g * half, (g + 1) * half)
        loads['ck', l, g].wait()
        s = dot(spread_queries(q), ck[rows]) * qk_scale
        e = jnp.exp(s - jnp.max(s, axis=-1, keepdims=True))
        w = e / jnp.sum(e, axis=-1, keepdims=True)
        loads['cv', l, g].wait()
        o = gather_heads(dot(cv[rows], w.T.astype(BF16))).astype(BF16)
        return dot(o, wout[l, 1])

    def mlp(l, g, hidden):
        f = dot(hidden, wfc1[l]) + b_fc1_ref[l:l + 1]
        act = (f * 0.5 * (1.0 + lax.erf(f * (2.0 ** -0.5)))).astype(BF16)
        return dot(act, wfc2[l])

    for l in range(LAYERS):
        first = 3 * l + 1
        for name in ('wqkv', 'sk', 'sv', 'wout'):
            loads[name, l].wait()
        new_rows = []
        for g in range(2):
            part_send[first - 1, g], new = attend_self(l, g, receive(first - 1, g))
            send(first, g)
            new_rows.append(new)
        for g in range(2):
            reduce(first, g, out_bias_ref[0, l:l + 1], *ln_of(l, 1))
        if l == 0:
            for key, c in loads.items():
                if key[1] > 0 and key[0] not in ('ck', 'cv'):
                    c.start()
            table_load.start()
        for g in range(2):
            write_new(l, g, *new_rows[g])
        loads['wcq', l].wait()
        for g in range(2):
            part_send[first, g] = attend_cross(l, g, receive(first, g))
            send(first + 1, g)
            if l + 1 < LAYERS:
                loads['ck', l + 1, g].start()
                loads['cv', l + 1, g].start()
        for g in range(2):
            reduce(first + 1, g, out_bias_ref[1, l:l + 1], *ln_of(l, 2))
        loads['fc1', l].wait()
        loads['fc2', l].wait()
        for g in range(2):
            part_send[first + 1, g] = mlp(l, g, receive(first + 1, g))
            send(first + 2, g)
        nxt = ln_of(l + 1, 0) if l + 1 < LAYERS else (lnf_ref[0:1], lnf_ref[1:2])
        for g in range(2):
            reduce(first + 2, g, out_bias_ref[2, l:l + 1], *nxt)

    last = N_PHASES - 1
    table_load.wait()
    h_out[...] = jnp.concatenate([receive(last, 0), receive(last, 1)], axis=0)

    for ph in range(N_PHASES):
        for g in range(2):
            @pl.when(me != OWNERS[g])
            def _():
                rs_copy(ph, g, me).wait_send()

            @pl.when(me == OWNERS[g])
            def _():
                for d in NEAR_FIRST[g]:
                    ag_copy(ph, g, d).wait_send()


def run_core(emb, pos, posn, in_bias, out_bias, b_fc1, ln_layers, ln_final, table, sk, sv, ck, cv, wqkv, wcq, wout, wfc1, wfc2):
    vm = pl.BlockSpec(memory_space=pltpu.VMEM)
    hbm = pl.BlockSpec(memory_space=pltpu.HBM)
    d_model = emb.shape[-1]
    smalls = (in_bias, out_bias, b_fc1, ln_layers, ln_final)
    n_loads = 11 * LAYERS + len(smalls) + 1
    return pl.pallas_call(
        core_kernel,
        out_shape=(pltpu.VMEM((BATCH, d_model), BF16),) + tuple(pltpu.VMEM(a.shape, BF16) for a in (table, sk, sv)),
        in_specs=[vm] * 3 + [hbm] * 15,
        out_specs=(vm,) * 4,
        scratch_shapes=[pltpu.VMEM(a.shape[1:], BF16) for a in (ck, cv)]
        + [pltpu.VMEM(a.shape, BF16) for a in (wqkv, wcq, wout, wfc1, wfc2)]
        + [pltpu.VMEM(a.shape, F32) for a in smalls]
        + [pltpu.VMEM((N_TP, ROWS, d_model), BF16),
           pltpu.VMEM((N_PHASES - 1, 2, ROWS, d_model), F32),
           pltpu.VMEM((N_PHASES - 1, N_TP, ROWS, d_model), F32),
           pltpu.VMEM((N_PHASES, 2, ROWS, d_model), BF16),
           pltpu.VMEM((ROWS, d_model), F32),
           pltpu.SemaphoreType.DMA((n_loads,)),
           pltpu.SemaphoreType.DMA((N_PHASES, 2)),
           pltpu.SemaphoreType.DMA((N_PHASES, N_TP)),
           pltpu.SemaphoreType.DMA((N_PHASES, N_TP)),
           pltpu.SemaphoreType.DMA((N_PHASES, 2))],
        compiler_params=pltpu.CompilerParams(collective_id=0, has_side_effects=True, vmem_limit_bytes=CORE_VMEM),
        cost_estimate=pl.CostEstimate(flops=4 << 30, bytes_accessed=150 << 20, transcendentals=0),
        name='decode_layers',
    )(emb, pos, posn, *in_hbm(in_bias, out_bias, b_fc1, ln_layers, ln_final, table, sk, sv, ck, cv, wqkv, wcq, wout, wfc1, wfc2))


def gather_kernel(tok_hbm, posn_hbm, table_hbm, pos_hbm, emb_out, pos_out, posn_out, emb_buf, pos_buf, tok_ref, pos_ref, sems, idx_sems):
    idx = [pltpu.make_async_copy(tok_hbm, tok_ref, idx_sems.at[0]), pltpu.make_async_copy(posn_hbm, pos_ref, idx_sems.at[1])]
    for c in idx:
        c.start()
    for c in idx:
        c.wait()
    shard_rows = table_hbm.shape[0]
    base = lax.axis_index('tp') * shard_rows
    copies = []
    for b in range(BATCH):
        row = jnp.clip(tok_ref[b] - base, 0, shard_rows - 1)
        at = pl.multiple_of((row // 8) * 8, 8)
        copies.append(pltpu.make_async_copy(table_hbm.at[pl.ds(at, 8)], emb_buf.at[pl.ds(b * 8, 8)], sems.at[0, b]))
        at = pl.multiple_of((pos_ref[b] // 8) * 8, 8)
        copies.append(pltpu.make_async_copy(pos_hbm.at[pl.ds(at, 8)], pos_buf.at[pl.ds(b * 8, 8)], sems.at[1, b]))
    for c in copies:
        c.start()
    row_i = lax.broadcasted_iota(jnp.int32, (BATCH, 8 * BATCH), 0)
    lane_i = lax.broadcasted_iota(jnp.int32, (BATCH, 8 * BATCH), 1)
    tok_at = jnp.zeros((BATCH, 8 * BATCH), jnp.int32)
    pos_at = jnp.zeros((BATCH, 8 * BATCH), jnp.int32)
    posn_row = lax.broadcasted_iota(jnp.int32, (BATCH, posn_out.shape[2]), 0)
    posn = jnp.zeros(posn_row.shape, jnp.int32)
    for b in range(BATCH):
        row = tok_ref[b] - base
        owned = (row >= 0) & (row < shard_rows)
        tok_at = jnp.where(row_i == b, jnp.where(owned, b * 8 + row % 8, -1), tok_at)
        pos_at = jnp.where(row_i == b, b * 8 + pos_ref[b] % 8, pos_at)
        posn = jnp.where(posn_row == b, pos_ref[b], posn)
    for g in range(2):
        posn_out[g] = jnp.concatenate([posn[g * ROWS:(g + 1) * ROWS]] * HEADS, axis=0)
    pick_tok = jnp.where(lane_i == tok_at, 1.0, 0.0).astype(BF16)
    pick_pos = jnp.where(lane_i == pos_at, 1.0, 0.0).astype(BF16)
    for c in copies:
        c.wait()
    emb = dot(pick_tok, emb_buf[...]).astype(BF16)
    pos = dot(pick_pos, pos_buf[...]).astype(BF16)
    for g in range(2):
        emb_out[g] = emb[g * ROWS:(g + 1) * ROWS]
        pos_out[g] = pos[g * ROWS:(g + 1) * ROWS]


def run_gather(tokens, positions, embed_table, pos_table, time):
    vm = pl.BlockSpec(memory_space=pltpu.VMEM)
    hbm = pl.BlockSpec(memory_space=pltpu.HBM)
    d_model = embed_table.shape[1]
    rows = pltpu.VMEM((2, ROWS, d_model), BF16)
    return pl.pallas_call(
        gather_kernel,
        out_shape=(rows, rows, pltpu.VMEM((2, HEADS * ROWS, time), jnp.int32)),
        in_specs=[hbm] * 4,
        out_specs=(vm, vm, vm),
        scratch_shapes=[pltpu.VMEM((8 * BATCH, d_model), BF16), pltpu.VMEM((8 * BATCH, d_model), BF16),
                        pltpu.SMEM((BATCH,), jnp.int32), pltpu.SMEM((BATCH,), jnp.int32),
                        pltpu.SemaphoreType.DMA((2, BATCH)), pltpu.SemaphoreType.DMA((2,))],
        compiler_params=pltpu.CompilerParams(vmem_limit_bytes=GATHER_VMEM),
        name='gather_rows',
    )(*in_hbm(tokens, positions, embed_table, pos_table))


N_TILES = 3


def final_kernel(h_ref, table_ref, sk_ref, sv_ref, logits_ref, sk_out, sv_out, sems):
    copies = [pltpu.make_async_copy(sk_ref, sk_out, sems.at[0]), pltpu.make_async_copy(sv_ref, sv_out, sems.at[1])]
    for c in copies:
        c.start()
    h_t = h_ref[...].astype(F32).T.astype(BF16)
    tile = table_ref.shape[0] // N_TILES
    for i in range(N_TILES):
        logits_ref[:, i * tile:(i + 1) * tile] = dot(table_ref[i * tile:(i + 1) * tile], h_t).T
    for c in copies:
        c.wait()


def run_final(hidden, table, sk, sv):
    vm = pl.BlockSpec(memory_space=pltpu.VMEM)
    hbm = pl.BlockSpec(memory_space=pltpu.HBM)
    cache = jax.ShapeDtypeStruct(sk.shape, BF16)
    return pl.pallas_call(
        final_kernel,
        out_shape=(jax.ShapeDtypeStruct((BATCH, table.shape[0]), F32), cache, cache),
        in_specs=[vm] * 4,
        out_specs=(vm, hbm, hbm),
        scratch_shapes=[pltpu.SemaphoreType.DMA((2,))],
        compiler_params=pltpu.CompilerParams(vmem_limit_bytes=FINAL_VMEM),
        name='logits_and_caches',
    )(hidden, table, sk, sv)


def solution(mesh):
    def local_step(tokens, positions, self_keys, self_vals, cross_keys, cross_vals, embed_table, pos_table, w_qkv, w_cq, in_bias, w_out, out_bias, w_fc1, b_fc1, w_fc2, ln_layers, ln_final):
        d_model = embed_table.shape[1]

        def rows_by_time(cache):
            return jnp.transpose(cache, (0, 1, 3, 4, 2)).reshape(LAYERS, BATCH * HD, cache.shape[2])

        def as_cache(rows):
            return jnp.transpose(rows.reshape(LAYERS, BATCH, HEADS, HEAD_DIM, rows.shape[2]), (0, 1, 4, 2, 3))

        sk, sv = rows_by_time(self_keys), rows_by_time(self_vals)
        emb, pos, posn = run_gather(tokens, positions, embed_table, pos_table, sk.shape[2])
        hidden, table, sk, sv = run_core(
            emb, pos, posn, in_bias, jnp.transpose(out_bias, (1, 0, 2)), b_fc1, ln_layers, ln_final,
            embed_table, sk, sv, rows_by_time(cross_keys), rows_by_time(cross_vals),
            jnp.transpose(w_qkv, (0, 2, 3, 4, 1)).reshape(LAYERS, 3 * HD, d_model),
            jnp.transpose(w_cq, (0, 2, 3, 1)).reshape(LAYERS, HD, d_model),
            w_out.reshape(LAYERS, 2, HD, d_model), w_fc1, w_fc2)
        logits, new_sk, new_sv = run_final(hidden, table, sk, sv)
        return logits, as_cache(new_sk), as_cache(new_sv)

    batch_spec = P('dp')
    cache_spec = P(None, 'dp', None, 'tp', None)
    in_specs = (batch_spec, batch_spec, cache_spec, cache_spec, cache_spec, cache_spec, P('tp', None), P(None, None), P(None, None, None, 'tp', None), P(None, None, 'tp', None), P(None, None, 'tp', None), P(None, None, 'tp', None, None), P(None, None, None), P(None, None, 'tp'), P(None, 'tp'), P(None, 'tp', None), P(None, None, None, None), P(None, None))
    out_specs = (P('dp', 'tp'), cache_spec, cache_spec)
    return jax.shard_map(local_step, mesh=mesh, in_specs=in_specs, out_specs=out_specs, check_vma=False)
```

```python
import functools

import jax
import jax.numpy as jnp
from jax import lax
from jax.experimental import pallas as pl
from jax.experimental.pallas import tpu as pltpu
from jax.sharding import PartitionSpec as P

BF16 = jnp.bfloat16
F32 = jnp.float32
MESH = pl.DeviceIdType.MESH
N_TP = 8
OWNERS = (3, 5)
NEAR_FIRST = (2, 1, 0, 5, 4, 7, 6)
ROWS = 8
BATCH = 16
HEADS = 2
HEAD_DIM = 64
HD = HEADS * HEAD_DIM
LAYERS = 2
GROUP_ROWS = 8 * 128
N_PHASES = 1 + 3 * LAYERS
CORE_VMEM = 30 << 20
GATHER_VMEM = 4 << 20
FINAL_VMEM = 6 << 20
NEG = -1e30


def dot(a, b):
    return jnp.dot(a, b, preferred_element_type=F32)


def dot_nt(a, b):
    return lax.dot_general(a, b, (((1,), (1,)), ((), ())), preferred_element_type=F32)


def in_hbm(*arrays):
    return tuple(pltpu.with_memory_space_constraint(a, pltpu.HBM) for a in arrays)


def layer_norm(x, gain, shift):
    mean = jnp.mean(x, axis=-1, keepdims=True)
    centred = x - mean
    var = jnp.mean(centred * centred, axis=-1, keepdims=True)
    return (centred * lax.rsqrt(var + 1e-5) * gain + shift).astype(BF16)


def head_row(ref, *idx):
    v = ref[idx]
    return jnp.concatenate([v[0:1], v[1:2]], axis=1)


def spread_queries(q):
    q2 = jnp.concatenate([q, q], axis=0)
    row = lax.broadcasted_iota(jnp.int32, q2.shape, 0)
    lane = lax.broadcasted_iota(jnp.int32, q2.shape, 1)
    q2 = jnp.where((row // ROWS) == (lane // HEAD_DIM), q2, 0.0)
    rb = row % ROWS
    return jnp.concatenate([jnp.where(rb == b, q2, 0.0).astype(BF16) for b in range(ROWS)], axis=1)


def gather_heads(mixed):
    col = lax.broadcasted_iota(jnp.int32, (HD, HEADS * ROWS), 1) % ROWS
    acc = jnp.zeros(col.shape, F32)
    for b in range(ROWS):
        acc = jnp.where(col == b, mixed[b * HD:(b + 1) * HD], acc)
    t = acc.T
    lane = lax.broadcasted_iota(jnp.int32, (ROWS, HD), 1)
    return jnp.where(lane < HEAD_DIM, t[:ROWS], t[ROWS:])


def core_kernel(emb_ref, pos_ref, posn_ref, in_bias_hbm, out_bias_hbm, b_fc1_hbm, ln_hbm, lnf_hbm,
                table_hbm, sk_hbm, sv_hbm, ck_hbm, cv_hbm, wqkv_hbm, wcq_hbm, wout_hbm, wfc1_hbm, wfc2_hbm,
                h_out, table, sk, sv,
                ck, cv, wqkv, wcq, wout, wfc1, wfc2,
                in_bias_ref, out_bias_ref, b_fc1_ref, ln_ref,
                emb_rs, part_send, part_rs, hbuf, x_ref, new_ref,
                small_sems, load_sems, half_sems, rs_send, rs_recv, ag_send, ag_recv):
    me = lax.axis_index('tp')
    n_ln = ln_hbm.shape[0]
    smalls = [(in_bias_hbm, in_bias_ref), (out_bias_hbm, out_bias_ref), (b_fc1_hbm, b_fc1_ref),
              (ln_hbm, ln_ref.at[pl.ds(0, n_ln)]), (lnf_hbm, ln_ref.at[pl.ds(n_ln, 1)])]
    small_loads = [pltpu.make_async_copy(src, dst, small_sems.at[i]) for i, (src, dst) in enumerate(smalls)]
    table_load = pltpu.make_async_copy(table_hbm, table, small_sems.at[len(smalls)])
    refs = {'wqkv': (wqkv_hbm, wqkv), 'sk': (sk_hbm, sk), 'sv': (sv_hbm, sv), 'wout': (wout_hbm, wout),
            'wcq': (wcq_hbm, wcq), 'fc1': (wfc1_hbm, wfc1), 'fc2': (wfc2_hbm, wfc2)}

    def load(name, l):
        src, dst = refs[name]
        return pltpu.make_async_copy(src.at[l], dst.at[l], load_sems.at[list(refs).index(name), l])

    def rows_of(g):
        return pl.ds(pl.multiple_of(g * GROUP_ROWS, GROUP_ROWS), GROUP_ROWS)

    def load_half(i, l, g):
        src, dst = ((ck_hbm, ck), (cv_hbm, cv))[i]
        return pltpu.make_async_copy(src.at[l, rows_of(g)], dst.at[rows_of(g)], half_sems.at[i, g])

    for c in small_loads:
        c.start()
    for name in ('wqkv', 'sk', 'sv', 'wout', 'wcq'):
        load(name, 0).start()
    for g in range(2):
        for i in range(2):
            load_half(i, 0, g).start()
    for name in ('fc1', 'fc2'):
        load(name, 0).start()

    barrier = pltpu.get_barrier_semaphore()
    is_owner = (me == OWNERS[0]) | (me == OWNERS[1])
    for d in range(N_TP):
        @pl.when((me != d) if d in OWNERS else is_owner)
        def _():
            pl.semaphore_signal(barrier, inc=1, device_id={'tp': d}, device_id_type=MESH)

    @pl.when(is_owner)
    def _():
        pl.semaphore_wait(barrier, N_TP - 1)

    @pl.when(jnp.logical_not(is_owner))
    def _():
        pl.semaphore_wait(barrier, 2)

    def owner_of(g):
        return OWNERS[0] + (OWNERS[1] - OWNERS[0]) * g

    def others(g):
        return [d + g * (N_TP - 2 - 2 * (d // 2) + d % 2 - d) for d in NEAR_FIRST]

    def rs_copy(ph, g, i):
        if isinstance(ph, int) and ph == 0:
            src, dst = emb_ref.at[g], emb_rs.at[i]
        else:
            src, dst = part_send.at[ph - 1, g], part_rs.at[ph - 1, i]
        return pltpu.make_async_remote_copy(src_ref=src, dst_ref=dst, send_sem=rs_send.at[ph, g], recv_sem=rs_recv.at[ph, i],
                                            device_id={'tp': owner_of(g)}, device_id_type=MESH)

    def ag_copy(ph, g, d):
        return pltpu.make_async_remote_copy(src_ref=hbuf.at[ph, g], dst_ref=hbuf.at[ph, g], send_sem=ag_send.at[ph, d], recv_sem=ag_recv.at[ph, g],
                                            device_id={'tp': d}, device_id_type=MESH)

    def send(ph, g):
        @pl.when(me != owner_of(g))
        def _():
            rs_copy(ph, g, me).start()

    def reduce(ph, bias):
        @pl.when(is_owner)
        def _():
            g = (me - OWNERS[0]) // (OWNERS[1] - OWNERS[0])
            first = bias is None
            total = (emb_ref[g] if first else part_send[ph - 1, g]).astype(F32)
            base = pos_ref[g].astype(F32) if first else x_ref[...] + bias
            for i in others(g):
                rs_copy(ph, g, i).wait_recv()
                total = total + (emb_rs[i] if first else part_rs[ph - 1, i]).astype(F32)
            x = total.astype(BF16).astype(F32) + base
            x_ref[...] = x
            hbuf[ph, g] = layer_norm(x, ln_ref[ph, 0:1], ln_ref[ph, 1:2])
            for d in reversed(others(g)):
                ag_copy(ph, g, d).start()

    def receive(ph, g):
        @pl.when(me != owner_of(g))
        def _():
            ag_copy(ph, g, 0).wait_recv()
        return hbuf[ph, g]

    for g in range(2):
        send(0, g)
    for c in small_loads:
        c.wait()
    reduce(0, None)

    time = sk.shape[2]
    qk_scale = HEAD_DIM ** -0.5

    def attend_self(l, g, hidden):
        qkv = dot_nt(hidden, wqkv[l])
        q = (qkv[:, :HD] + head_row(in_bias_ref, l, 0)).astype(BF16).astype(F32)
        k_new = qkv[:, HD:2 * HD].astype(BF16).astype(F32)
        v_new = (qkv[:, 2 * HD:] + head_row(in_bias_ref, l, 1)).astype(BF16).astype(F32)
        new_ref[0, g] = k_new
        new_ref[1, g] = v_new
        prod = q * k_new
        s_new = jnp.concatenate([jnp.sum(prod[:, :HEAD_DIM], axis=1, keepdims=True), jnp.sum(prod[:, HEAD_DIM:], axis=1, keepdims=True)], axis=0)
        posn = posn_ref[g]
        t_idx = lax.broadcasted_iota(jnp.int32, posn.shape, 1)
        here = t_idx == posn
        s = jnp.where(here, s_new, dot(spread_queries(q), sk[l, rows_of(g)])) * qk_scale
        s = jnp.where(t_idx <= posn, s, NEG)
        e = jnp.exp(s - jnp.max(s, axis=-1, keepdims=True))
        w = (e / jnp.sum(e, axis=-1, keepdims=True)).astype(BF16).astype(F32)
        w_new = jnp.sum(jnp.where(here, w, 0.0), axis=-1, keepdims=True)
        w_old = jnp.where(here, 0.0, w)
        mixed = gather_heads(dot(sv[l, rows_of(g)], w_old.T.astype(BF16)))
        lane = lax.broadcasted_iota(jnp.int32, (ROWS, HD), 1)
        w_row = jnp.where(lane < HEAD_DIM, w_new[:ROWS], w_new[ROWS:])
        o = (mixed + w_row * v_new).astype(BF16)
        return dot(o, wout[l, 0])

    def write_new(l, g):
        t_row = lax.broadcasted_iota(jnp.int32, (HD, time), 1)
        cols = [new_ref[i, g].T for i in range(2)]
        for b in range(ROWS):
            at = t_row == posn_ref[g, b:b + 1]
            rows = pl.ds(pl.multiple_of(g * GROUP_ROWS + b * HD, HD), HD)
            for ref, col in zip((sk, sv), cols):
                ref[l, rows] = jnp.where(at, col[:, b:b + 1], ref[l, rows].astype(F32)).astype(BF16)

    def attend_cross(l, g, hidden):
        q = (dot_nt(hidden, wcq[l]) + head_row(in_bias_ref, l, 2)).astype(BF16).astype(F32)
        load_half(0, l, g).wait()
        s = dot(spread_queries(q), ck[rows_of(g)]) * qk_scale
        e = jnp.exp(s - jnp.max(s, axis=-1, keepdims=True))
        w = e / jnp.sum(e, axis=-1, keepdims=True)
        load_half(1, l, g).wait()
        o = gather_heads(dot(cv[rows_of(g)], w.T.astype(BF16))).astype(BF16)
        return dot(o, wout[l, 1])

    def mlp(l, g, hidden):
        f = dot(hidden, wfc1[l]) + b_fc1_ref[pl.ds(l, 1)]
        act = (f * 0.5 * (1.0 + lax.erf(f * (2.0 ** -0.5)))).astype(BF16)
        return dot(act, wfc2[l])

    def both_streams(body):
        lax.fori_loop(0, 2, lambda g, c: (body(g), c)[1], 0)

    def layer(l, carry):
        ph = 3 * l + 1

        def block(ph, compute, after=None):
            def stream(g):
                part_send[ph - 1, g] = compute(l, g, receive(ph - 1, g))
                send(ph, g)
                if after is not None:
                    after(g)
            both_streams(stream)

        for name in ('wqkv', 'sk', 'sv', 'wout'):
            load(name, l).wait()
        block(ph, attend_self)
        reduce(ph, out_bias_ref[0, pl.ds(l, 1)])

        @pl.when(l == 0)
        def _():
            for name in refs:
                for k in range(1, LAYERS):
                    load(name, k).start()
            table_load.start()

        both_streams(lambda g: write_new(l, g))
        load('wcq', l).wait()

        def next_half(g):
            @pl.when(l + 1 < LAYERS)
            def _():
                for i in range(2):
                    load_half(i, l + 1, g).start()

        block(ph + 1, attend_cross, next_half)
        reduce(ph + 1, out_bias_ref[1, pl.ds(l, 1)])
        load('fc1', l).wait()
        load('fc2', l).wait()
        block(ph + 2, mlp)
        reduce(ph + 2, out_bias_ref[2, pl.ds(l, 1)])
        return carry

    lax.fori_loop(0, LAYERS, layer, 0)
    last = N_PHASES - 1
    table_load.wait()
    h_out[...] = jnp.concatenate([receive(last, 0), receive(last, 1)], axis=0)

    def drain(ph, carry):
        for g in range(2):
            @pl.when(me != OWNERS[g])
            def _():
                rs_copy(ph, g, me).wait_send()

        @pl.when(is_owner)
        def _():
            g = (me - OWNERS[0]) // (OWNERS[1] - OWNERS[0])
            for d in others(g):
                ag_copy(ph, g, d).wait_send()
        return carry

    for g in range(2):
        @pl.when(me != OWNERS[g])
        def _():
            rs_copy(0, g, me).wait_send()

    @pl.when(is_owner)
    def _():
        g = (me - OWNERS[0]) // (OWNERS[1] - OWNERS[0])
        for d in others(g):
            ag_copy(0, g, d).wait_send()

    lax.fori_loop(1, N_PHASES, drain, 0)


def run_core(emb, pos, posn, in_bias, out_bias, b_fc1, ln_layers, ln_final, table, sk, sv, ck, cv, wqkv, wcq, wout, wfc1, wfc2):
    vm = pl.BlockSpec(memory_space=pltpu.VMEM)
    hbm = pl.BlockSpec(memory_space=pltpu.HBM)
    d_model = emb.shape[-1]
    ln_rows = ln_layers.shape[0] + 1
    return pl.pallas_call(
        core_kernel,
        out_shape=(pltpu.VMEM((BATCH, d_model), BF16),) + tuple(pltpu.VMEM(a.shape, BF16) for a in (table, sk, sv)),
        in_specs=[vm] * 3 + [hbm] * 15,
        out_specs=(vm,) * 4,
        scratch_shapes=[pltpu.VMEM(a.shape[1:], BF16) for a in (ck, cv)]
        + [pltpu.VMEM(a.shape, BF16) for a in (wqkv, wcq, wout, wfc1, wfc2)]
        + [pltpu.VMEM(a.shape, F32) for a in (in_bias, out_bias, b_fc1)]
        + [pltpu.VMEM((ln_rows, 2, d_model), F32),
           pltpu.VMEM((N_TP, ROWS, d_model), BF16),
           pltpu.VMEM((N_PHASES - 1, 2, ROWS, d_model), F32),
           pltpu.VMEM((N_PHASES - 1, N_TP, ROWS, d_model), F32),
           pltpu.VMEM((N_PHASES, 2, ROWS, d_model), BF16),
           pltpu.VMEM((ROWS, d_model), F32),
           pltpu.VMEM((2, 2, ROWS, HD), F32),
           pltpu.SemaphoreType.DMA((6,)),
           pltpu.SemaphoreType.DMA((7, LAYERS)),
           pltpu.SemaphoreType.DMA((2, 2)),
           pltpu.SemaphoreType.DMA((N_PHASES, 2)),
           pltpu.SemaphoreType.DMA((N_PHASES, N_TP)),
           pltpu.SemaphoreType.DMA((N_PHASES, N_TP)),
           pltpu.SemaphoreType.DMA((N_PHASES, 2))],
        compiler_params=pltpu.CompilerParams(collective_id=0, has_side_effects=True, vmem_limit_bytes=CORE_VMEM),
        cost_estimate=pl.CostEstimate(flops=4 << 30, bytes_accessed=150 << 20, transcendentals=0),
        name='decode_layers',
    )(emb, pos, posn, *in_hbm(in_bias, out_bias, b_fc1, ln_layers, ln_final, table, sk, sv, ck, cv, wqkv, wcq, wout, wfc1, wfc2))


def gather_kernel(tok_hbm, posn_hbm, table_hbm, pos_hbm, emb_out, pos_out, posn_out, emb_buf, pos_buf, tok_ref, pos_ref, sems, idx_sems):
    idx = [pltpu.make_async_copy(tok_hbm, tok_ref, idx_sems.at[0]), pltpu.make_async_copy(posn_hbm, pos_ref, idx_sems.at[1])]
    for c in idx:
        c.start()
    for c in idx:
        c.wait()
    shard_rows = table_hbm.shape[0]
    base = lax.axis_index('tp') * shard_rows
    copies = []
    for b in range(BATCH):
        row = jnp.clip(tok_ref[b] - base, 0, shard_rows - 1)
        at = pl.multiple_of((row // 8) * 8, 8)
        copies.append(pltpu.make_async_copy(table_hbm.at[pl.ds(at, 8)], emb_buf.at[pl.ds(b * 8, 8)], sems.at[0, b]))
        at = pl.multiple_of((pos_ref[b] // 8) * 8, 8)
        copies.append(pltpu.make_async_copy(pos_hbm.at[pl.ds(at, 8)], pos_buf.at[pl.ds(b * 8, 8)], sems.at[1, b]))
    for c in copies:
        c.start()
    row_i = lax.broadcasted_iota(jnp.int32, (BATCH, 8 * BATCH), 0)
    lane_i = lax.broadcasted_iota(jnp.int32, (BATCH, 8 * BATCH), 1)
    tok_at = jnp.zeros((BATCH, 8 * BATCH), jnp.int32)
    pos_at = jnp.zeros((BATCH, 8 * BATCH), jnp.int32)
    posn_row = lax.broadcasted_iota(jnp.int32, (BATCH, posn_out.shape[2]), 0)
    posn = jnp.zeros(posn_row.shape, jnp.int32)
    for b in range(BATCH):
        row = tok_ref[b] - base
        owned = (row >= 0) & (row < shard_rows)
        tok_at = jnp.where(row_i == b, jnp.where(owned, b * 8 + row % 8, -1), tok_at)
        pos_at = jnp.where(row_i == b, b * 8 + pos_ref[b] % 8, pos_at)
        posn = jnp.where(posn_row == b, pos_ref[b], posn)
    for g in range(2):
        posn_out[g] = jnp.concatenate([posn[g * ROWS:(g + 1) * ROWS]] * HEADS, axis=0)
    pick_tok = jnp.where(lane_i == tok_at, 1.0, 0.0).astype(BF16)
    pick_pos = jnp.where(lane_i == pos_at, 1.0, 0.0).astype(BF16)
    for c in copies:
        c.wait()
    emb = dot(pick_tok, emb_buf[...]).astype(BF16)
    pos = dot(pick_pos, pos_buf[...]).astype(BF16)
    for g in range(2):
        emb_out[g] = emb[g * ROWS:(g + 1) * ROWS]
        pos_out[g] = pos[g * ROWS:(g + 1) * ROWS]


def run_gather(tokens, positions, embed_table, pos_table, time):
    vm = pl.BlockSpec(memory_space=pltpu.VMEM)
    hbm = pl.BlockSpec(memory_space=pltpu.HBM)
    d_model = embed_table.shape[1]
    rows = pltpu.VMEM((2, ROWS, d_model), BF16)
    return pl.pallas_call(
        gather_kernel,
        out_shape=(rows, rows, pltpu.VMEM((2, HEADS * ROWS, time), jnp.int32)),
        in_specs=[hbm] * 4,
        out_specs=(vm, vm, vm),
        scratch_shapes=[pltpu.VMEM((8 * BATCH, d_model), BF16), pltpu.VMEM((8 * BATCH, d_model), BF16),
                        pltpu.SMEM((BATCH,), jnp.int32), pltpu.SMEM((BATCH,), jnp.int32),
                        pltpu.SemaphoreType.DMA((2, BATCH)), pltpu.SemaphoreType.DMA((2,))],
        compiler_params=pltpu.CompilerParams(vmem_limit_bytes=GATHER_VMEM),
        name='gather_rows',
    )(*in_hbm(tokens, positions, embed_table, pos_table))


N_TILES = 3


def final_kernel(h_ref, table_ref, sk_ref, sv_ref, logits_ref, sk_out, sv_out, sems):
    copies = [pltpu.make_async_copy(sk_ref, sk_out, sems.at[0]), pltpu.make_async_copy(sv_ref, sv_out, sems.at[1])]
    for c in copies:
        c.start()
    h_t = h_ref[...].astype(F32).T.astype(BF16)
    tile = table_ref.shape[0] // N_TILES
    for i in range(N_TILES):
        logits_ref[:, i * tile:(i + 1) * tile] = dot(table_ref[i * tile:(i + 1) * tile], h_t).T
    for c in copies:
        c.wait()


def run_final(hidden, table, sk, sv):
    vm = pl.BlockSpec(memory_space=pltpu.VMEM)
    hbm = pl.BlockSpec(memory_space=pltpu.HBM)
    cache = jax.ShapeDtypeStruct(sk.shape, BF16)
    return pl.pallas_call(
        final_kernel,
        out_shape=(jax.ShapeDtypeStruct((BATCH, table.shape[0]), F32), cache, cache),
        in_specs=[vm] * 4,
        out_specs=(vm, hbm, hbm),
        scratch_shapes=[pltpu.SemaphoreType.DMA((2,))],
        compiler_params=pltpu.CompilerParams(vmem_limit_bytes=FINAL_VMEM),
        name='logits_and_caches',
    )(hidden, table, sk, sv)


def solution(mesh):
    def local_step(tokens, positions, self_keys, self_vals, cross_keys, cross_vals, embed_table, pos_table, w_qkv, w_cq, in_bias, w_out, out_bias, w_fc1, b_fc1, w_fc2, ln_layers, ln_final):
        d_model = embed_table.shape[1]

        def rows_by_time(cache):
            return jnp.transpose(cache, (0, 1, 3, 4, 2)).reshape(LAYERS, BATCH * HD, cache.shape[2])

        def as_cache(rows):
            return jnp.transpose(rows.reshape(LAYERS, BATCH, HEADS, HEAD_DIM, rows.shape[2]), (0, 1, 4, 2, 3))

        sk, sv = rows_by_time(self_keys), rows_by_time(self_vals)
        emb, pos, posn = run_gather(tokens, positions, embed_table, pos_table, sk.shape[2])
        hidden, table, sk, sv = run_core(
            emb, pos, posn, in_bias, jnp.transpose(out_bias, (1, 0, 2)), b_fc1, ln_layers.reshape(-1, 2, d_model), ln_final[None],
            embed_table, sk, sv, rows_by_time(cross_keys), rows_by_time(cross_vals),
            jnp.transpose(w_qkv, (0, 2, 3, 4, 1)).reshape(LAYERS, 3 * HD, d_model),
            jnp.transpose(w_cq, (0, 2, 3, 1)).reshape(LAYERS, HD, d_model),
            w_out.reshape(LAYERS, 2, HD, d_model), w_fc1, w_fc2)
        logits, new_sk, new_sv = run_final(hidden, table, sk, sv)
        return logits, as_cache(new_sk), as_cache(new_sv)

    batch_spec = P('dp')
    cache_spec = P(None, 'dp', None, 'tp', None)
    in_specs = (batch_spec, batch_spec, cache_spec, cache_spec, cache_spec, cache_spec, P('tp', None), P(None, None), P(None, None, None, 'tp', None), P(None, None, 'tp', None), P(None, None, 'tp', None), P(None, None, 'tp', None, None), P(None, None, None), P(None, None, 'tp'), P(None, 'tp'), P(None, 'tp', None), P(None, None, None, None), P(None, None))
    out_specs = (P('dp', 'tp'), cache_spec, cache_spec)
    return jax.shard_map(local_step, mesh=mesh, in_specs=in_specs, out_specs=out_specs, check_vma=False)
```

```python
import functools

import jax
import jax.numpy as jnp
from jax import lax
from jax.experimental import pallas as pl
from jax.experimental.pallas import tpu as pltpu
from jax.sharding import PartitionSpec as P

BF16 = jnp.bfloat16
F32 = jnp.float32
MESH = pl.DeviceIdType.MESH
N_TP = 8
OWNERS = (3, 5)
NEAR_FIRST = (2, 1, 0, 5, 4, 7, 6)
ROWS = 8
BATCH = 16
HEADS = 2
HEAD_DIM = 64
HD = HEADS * HEAD_DIM
LAYERS = 2
GROUP_ROWS = 8 * 128
N_PHASES = 1 + 3 * LAYERS
CORE_VMEM = 30 << 20
GATHER_VMEM = 4 << 20
FINAL_VMEM = 6 << 20
NEG = -1e30


def dot(a, b):
    return jnp.dot(a, b, preferred_element_type=F32)


def dot_nt(a, b):
    return lax.dot_general(a, b, (((1,), (1,)), ((), ())), preferred_element_type=F32)


def in_hbm(*arrays):
    return tuple(pltpu.with_memory_space_constraint(a, pltpu.HBM) for a in arrays)


def layer_norm(x, gain, shift):
    mean = jnp.mean(x, axis=-1, keepdims=True)
    centred = x - mean
    var = jnp.mean(centred * centred, axis=-1, keepdims=True)
    return (centred * lax.rsqrt(var + 1e-5) * gain + shift).astype(BF16)


def head_row(ref, *idx):
    v = ref[idx]
    return jnp.concatenate([v[0:1], v[1:2]], axis=1)


def spread_queries(q):
    q2 = jnp.concatenate([q, q], axis=0)
    row = lax.broadcasted_iota(jnp.int32, q2.shape, 0)
    lane = lax.broadcasted_iota(jnp.int32, q2.shape, 1)
    q2 = jnp.where((row // ROWS) == (lane // HEAD_DIM), q2, 0.0)
    rb = row % ROWS
    return jnp.concatenate([jnp.where(rb == b, q2, 0.0).astype(BF16) for b in range(ROWS)], axis=1)


def gather_heads(mixed):
    row = lax.broadcasted_iota(jnp.int32, (HEADS * ROWS, HD), 0) % ROWS
    acc = jnp.zeros(row.shape, F32)
    for b in range(ROWS):
        acc = jnp.where(row == b, mixed[:, b * HD:(b + 1) * HD], acc)
    lane = lax.broadcasted_iota(jnp.int32, (ROWS, HD), 1)
    return jnp.where(lane < HEAD_DIM, acc[:ROWS], acc[ROWS:])


def core_kernel(emb_ref, pos_ref, posn_ref, in_bias_hbm, out_bias_hbm, b_fc1_hbm, ln_hbm, lnf_hbm,
                table_hbm, sk_hbm, sv_hbm, ck_hbm, cv_hbm, wqkv_hbm, wcq_hbm, wout_hbm, wfc1_hbm, wfc2_hbm,
                h_out, table, sk, sv,
                ck, cv, wqkv, wcq, wout, wfc1, wfc2,
                in_bias_ref, out_bias_ref, b_fc1_ref, ln_ref,
                emb_rs, part_send, part_rs, hbuf, x_ref, new_ref,
                small_sems, load_sems, half_sems, rs_send, rs_recv, ag_send, ag_recv):
    me = lax.axis_index('tp')
    n_ln = ln_hbm.shape[0]
    smalls = [(in_bias_hbm, in_bias_ref), (out_bias_hbm, out_bias_ref), (b_fc1_hbm, b_fc1_ref),
              (ln_hbm, ln_ref.at[pl.ds(0, n_ln)]), (lnf_hbm, ln_ref.at[pl.ds(n_ln, 1)])]
    small_loads = [pltpu.make_async_copy(src, dst, small_sems.at[i]) for i, (src, dst) in enumerate(smalls)]
    table_load = pltpu.make_async_copy(table_hbm, table, small_sems.at[len(smalls)])
    refs = {'wqkv': (wqkv_hbm, wqkv), 'sk': (sk_hbm, sk), 'sv': (sv_hbm, sv), 'wout': (wout_hbm, wout),
            'wcq': (wcq_hbm, wcq), 'fc1': (wfc1_hbm, wfc1), 'fc2': (wfc2_hbm, wfc2)}

    def load(name, l):
        src, dst = refs[name]
        return pltpu.make_async_copy(src.at[l], dst.at[l], load_sems.at[list(refs).index(name), l])

    def rows_of(g):
        return pl.ds(pl.multiple_of(g * GROUP_ROWS, GROUP_ROWS), GROUP_ROWS)

    def load_half(i, l, g):
        src, dst = ((ck_hbm, ck), (cv_hbm, cv))[i]
        return pltpu.make_async_copy(src.at[l, rows_of(g)], dst.at[rows_of(g)], half_sems.at[i, g])

    for c in small_loads:
        c.start()
    for name in ('wqkv', 'sk', 'sv', 'wout', 'wcq'):
        load(name, 0).start()
    for g in range(2):
        for i in range(2):
            load_half(i, 0, g).start()
    for name in ('fc1', 'fc2'):
        load(name, 0).start()

    barrier = pltpu.get_barrier_semaphore()
    is_owner = (me == OWNERS[0]) | (me == OWNERS[1])
    for d in range(N_TP):
        @pl.when((me != d) if d in OWNERS else is_owner)
        def _():
            pl.semaphore_signal(barrier, inc=1, device_id={'tp': d}, device_id_type=MESH)

    @pl.when(is_owner)
    def _():
        pl.semaphore_wait(barrier, N_TP - 1)

    @pl.when(jnp.logical_not(is_owner))
    def _():
        pl.semaphore_wait(barrier, 2)

    def owner_of(g):
        return OWNERS[0] + (OWNERS[1] - OWNERS[0]) * g

    def others(g):
        return [d + g * (N_TP - 2 - 2 * (d // 2) + d % 2 - d) for d in NEAR_FIRST]

    def rs_copy(ph, g, i):
        if isinstance(ph, int) and ph == 0:
            src, dst = emb_ref.at[g], emb_rs.at[i]
        else:
            src, dst = part_send.at[ph - 1, g], part_rs.at[ph - 1, i]
        return pltpu.make_async_remote_copy(src_ref=src, dst_ref=dst, send_sem=rs_send.at[ph, g], recv_sem=rs_recv.at[ph, i],
                                            device_id={'tp': owner_of(g)}, device_id_type=MESH)

    def ag_copy(ph, g, d):
        return pltpu.make_async_remote_copy(src_ref=hbuf.at[ph, g], dst_ref=hbuf.at[ph, g], send_sem=ag_send.at[ph, d], recv_sem=ag_recv.at[ph, g],
                                            device_id={'tp': d}, device_id_type=MESH)

    def send(ph, g):
        @pl.when(me != owner_of(g))
        def _():
            rs_copy(ph, g, me).start()

    def reduce(ph, bias):
        @pl.when(is_owner)
        def _():
            g = (me - OWNERS[0]) // (OWNERS[1] - OWNERS[0])
            first = bias is None
            total = (emb_ref[g] if first else part_send[ph - 1, g]).astype(F32)
            base = pos_ref[g].astype(F32) if first else x_ref[...] + bias
            for i in others(g):
                rs_copy(ph, g, i).wait_recv()
                total = total + (emb_rs[i] if first else part_rs[ph - 1, i]).astype(F32)
            x = total.astype(BF16).astype(F32) + base
            x_ref[...] = x
            hbuf[ph, g] = layer_norm(x, ln_ref[ph, 0:1], ln_ref[ph, 1:2])
            for d in reversed(others(g)):
                ag_copy(ph, g, d).start()

    def receive(ph, g):
        @pl.when(me != owner_of(g))
        def _():
            ag_copy(ph, g, 0).wait_recv()
        return hbuf[ph, g]

    for g in range(2):
        send(0, g)
    for c in small_loads:
        c.wait()
    reduce(0, None)

    time = sk.shape[2]
    qk_scale = HEAD_DIM ** -0.5

    def attend_self(l, g, hidden):
        qkv = dot_nt(hidden, wqkv[l])
        q = (qkv[:, :HD] + head_row(in_bias_ref, l, 0)).astype(BF16).astype(F32)
        k_new = qkv[:, HD:2 * HD].astype(BF16).astype(F32)
        v_new = (qkv[:, 2 * HD:] + head_row(in_bias_ref, l, 1)).astype(BF16).astype(F32)
        new_ref[0, g] = k_new
        new_ref[1, g] = v_new
        prod = q * k_new
        s_new = jnp.concatenate([jnp.sum(prod[:, :HEAD_DIM], axis=1, keepdims=True), jnp.sum(prod[:, HEAD_DIM:], axis=1, keepdims=True)], axis=0)
        posn = posn_ref[g]
        t_idx = lax.broadcasted_iota(jnp.int32, posn.shape, 1)
        here = t_idx == posn
        s = jnp.where(here, s_new, dot(spread_queries(q), sk[l, rows_of(g)])) * qk_scale
        s = jnp.where(t_idx <= posn, s, NEG)
        e = jnp.exp(s - jnp.max(s, axis=-1, keepdims=True))
        w = (e / jnp.sum(e, axis=-1, keepdims=True)).astype(BF16).astype(F32)
        w_new = jnp.sum(jnp.where(here, w, 0.0), axis=-1, keepdims=True)
        w_old = jnp.where(here, 0.0, w)
        mixed = gather_heads(dot_nt(w_old.astype(BF16), sv[l, rows_of(g)]))
        lane = lax.broadcasted_iota(jnp.int32, (ROWS, HD), 1)
        w_row = jnp.where(lane < HEAD_DIM, w_new[:ROWS], w_new[ROWS:])
        o = (mixed + w_row * v_new).astype(BF16)
        return dot(o, wout[l, 0])

    def write_new(l, g):
        t_row = lax.broadcasted_iota(jnp.int32, (HD, time), 1)
        cols = [new_ref[i, g].T for i in range(2)]
        for b in range(ROWS):
            at = t_row == posn_ref[g, b:b + 1]
            rows = pl.ds(pl.multiple_of(g * GROUP_ROWS + b * HD, HD), HD)
            for ref, col in zip((sk, sv), cols):
                ref[l, rows] = jnp.where(at, col[:, b:b + 1], ref[l, rows].astype(F32)).astype(BF16)

    def attend_cross(l, g, hidden):
        q = (dot_nt(hidden, wcq[l]) + head_row(in_bias_ref, l, 2)).astype(BF16).astype(F32)
        load_half(0, l, g).wait()
        s = dot(spread_queries(q), ck[rows_of(g)]) * qk_scale
        e = jnp.exp(s - jnp.max(s, axis=-1, keepdims=True))
        w = e / jnp.sum(e, axis=-1, keepdims=True)
        load_half(1, l, g).wait()
        o = gather_heads(dot_nt(w.astype(BF16), cv[rows_of(g)])).astype(BF16)
        return dot(o, wout[l, 1])

    def mlp(l, g, hidden):
        f = dot(hidden, wfc1[l]) + b_fc1_ref[pl.ds(l, 1)]
        act = (f * 0.5 * (1.0 + lax.erf(f * (2.0 ** -0.5)))).astype(BF16)
        return dot(act, wfc2[l])

    def both_streams(body):
        lax.fori_loop(0, 2, lambda g, c: (body(g), c)[1], 0)

    def layer(l, carry):
        ph = 3 * l + 1

        def block(ph, compute, after=None):
            def stream(g):
                part_send[ph - 1, g] = compute(l, g, receive(ph - 1, g))
                send(ph, g)
                if after is not None:
                    after(g)
            both_streams(stream)

        for name in ('wqkv', 'sk', 'sv', 'wout'):
            load(name, l).wait()
        block(ph, attend_self)
        reduce(ph, out_bias_ref[0, pl.ds(l, 1)])

        @pl.when(l == 0)
        def _():
            for name in refs:
                for k in range(1, LAYERS):
                    load(name, k).start()
            table_load.start()

        both_streams(lambda g: write_new(l, g))
        load('wcq', l).wait()

        def next_half(g):
            @pl.when(l + 1 < LAYERS)
            def _():
                for i in range(2):
                    load_half(i, l + 1, g).start()

        block(ph + 1, attend_cross, next_half)
        reduce(ph + 1, out_bias_ref[1, pl.ds(l, 1)])
        load('fc1', l).wait()
        load('fc2', l).wait()
        block(ph + 2, mlp)
        reduce(ph + 2, out_bias_ref[2, pl.ds(l, 1)])
        return carry

    lax.fori_loop(0, LAYERS, layer, 0)
    last = N_PHASES - 1
    table_load.wait()
    h_out[...] = jnp.concatenate([receive(last, 0), receive(last, 1)], axis=0)

    def drain(ph, carry):
        for g in range(2):
            @pl.when(me != OWNERS[g])
            def _():
                rs_copy(ph, g, me).wait_send()

        @pl.when(is_owner)
        def _():
            g = (me - OWNERS[0]) // (OWNERS[1] - OWNERS[0])
            for d in others(g):
                ag_copy(ph, g, d).wait_send()
        return carry

    for g in range(2):
        @pl.when(me != OWNERS[g])
        def _():
            rs_copy(0, g, me).wait_send()

    @pl.when(is_owner)
    def _():
        g = (me - OWNERS[0]) // (OWNERS[1] - OWNERS[0])
        for d in others(g):
            ag_copy(0, g, d).wait_send()

    lax.fori_loop(1, N_PHASES, drain, 0)


def run_core(emb, pos, posn, in_bias, out_bias, b_fc1, ln_layers, ln_final, table, sk, sv, ck, cv, wqkv, wcq, wout, wfc1, wfc2):
    vm = pl.BlockSpec(memory_space=pltpu.VMEM)
    hbm = pl.BlockSpec(memory_space=pltpu.HBM)
    d_model = emb.shape[-1]
    ln_rows = ln_layers.shape[0] + 1
    return pl.pallas_call(
        core_kernel,
        out_shape=(pltpu.VMEM((BATCH, d_model), BF16),) + tuple(pltpu.VMEM(a.shape, BF16) for a in (table, sk, sv)),
        in_specs=[vm] * 3 + [hbm] * 15,
        out_specs=(vm,) * 4,
        scratch_shapes=[pltpu.VMEM(a.shape[1:], BF16) for a in (ck, cv)]
        + [pltpu.VMEM(a.shape, BF16) for a in (wqkv, wcq, wout, wfc1, wfc2)]
        + [pltpu.VMEM(a.shape, F32) for a in (in_bias, out_bias, b_fc1)]
        + [pltpu.VMEM((ln_rows, 2, d_model), F32),
           pltpu.VMEM((N_TP, ROWS, d_model), BF16),
           pltpu.VMEM((N_PHASES - 1, 2, ROWS, d_model), F32),
           pltpu.VMEM((N_PHASES - 1, N_TP, ROWS, d_model), F32),
           pltpu.VMEM((N_PHASES, 2, ROWS, d_model), BF16),
           pltpu.VMEM((ROWS, d_model), F32),
           pltpu.VMEM((2, 2, ROWS, HD), F32),
           pltpu.SemaphoreType.DMA((6,)),
           pltpu.SemaphoreType.DMA((7, LAYERS)),
           pltpu.SemaphoreType.DMA((2, 2)),
           pltpu.SemaphoreType.DMA((N_PHASES, 2)),
           pltpu.SemaphoreType.DMA((N_PHASES, N_TP)),
           pltpu.SemaphoreType.DMA((N_PHASES, N_TP)),
           pltpu.SemaphoreType.DMA((N_PHASES, 2))],
        compiler_params=pltpu.CompilerParams(collective_id=0, has_side_effects=True, vmem_limit_bytes=CORE_VMEM),
        cost_estimate=pl.CostEstimate(flops=4 << 30, bytes_accessed=150 << 20, transcendentals=0),
        name='decode_layers',
    )(emb, pos, posn, *in_hbm(in_bias, out_bias, b_fc1, ln_layers, ln_final, table, sk, sv, ck, cv, wqkv, wcq, wout, wfc1, wfc2))


def gather_kernel(tok_hbm, posn_hbm, table_hbm, pos_hbm, emb_out, pos_out, posn_out, emb_buf, pos_buf, tok_ref, pos_ref, sems, idx_sems):
    idx = [pltpu.make_async_copy(tok_hbm, tok_ref, idx_sems.at[0]), pltpu.make_async_copy(posn_hbm, pos_ref, idx_sems.at[1])]
    for c in idx:
        c.start()
    for c in idx:
        c.wait()
    shard_rows = table_hbm.shape[0]
    base = lax.axis_index('tp') * shard_rows
    copies = []
    for b in range(BATCH):
        row = jnp.clip(tok_ref[b] - base, 0, shard_rows - 1)
        at = pl.multiple_of((row // 8) * 8, 8)
        copies.append(pltpu.make_async_copy(table_hbm.at[pl.ds(at, 8)], emb_buf.at[pl.ds(b * 8, 8)], sems.at[0, b]))
        at = pl.multiple_of((pos_ref[b] // 8) * 8, 8)
        copies.append(pltpu.make_async_copy(pos_hbm.at[pl.ds(at, 8)], pos_buf.at[pl.ds(b * 8, 8)], sems.at[1, b]))
    for c in copies:
        c.start()
    row_i = lax.broadcasted_iota(jnp.int32, (BATCH, 8 * BATCH), 0)
    lane_i = lax.broadcasted_iota(jnp.int32, (BATCH, 8 * BATCH), 1)
    tok_at = jnp.zeros((BATCH, 8 * BATCH), jnp.int32)
    pos_at = jnp.zeros((BATCH, 8 * BATCH), jnp.int32)
    posn_row = lax.broadcasted_iota(jnp.int32, (BATCH, posn_out.shape[2]), 0)
    posn = jnp.zeros(posn_row.shape, jnp.int32)
    for b in range(BATCH):
        row = tok_ref[b] - base
        owned = (row >= 0) & (row < shard_rows)
        tok_at = jnp.where(row_i == b, jnp.where(owned, b * 8 + row % 8, -1), tok_at)
        pos_at = jnp.where(row_i == b, b * 8 + pos_ref[b] % 8, pos_at)
        posn = jnp.where(posn_row == b, pos_ref[b], posn)
    for g in range(2):
        posn_out[g] = jnp.concatenate([posn[g * ROWS:(g + 1) * ROWS]] * HEADS, axis=0)
    pick_tok = jnp.where(lane_i == tok_at, 1.0, 0.0).astype(BF16)
    pick_pos = jnp.where(lane_i == pos_at, 1.0, 0.0).astype(BF16)
    for c in copies:
        c.wait()
    emb = dot(pick_tok, emb_buf[...]).astype(BF16)
    pos = dot(pick_pos, pos_buf[...]).astype(BF16)
    for g in range(2):
        emb_out[g] = emb[g * ROWS:(g + 1) * ROWS]
        pos_out[g] = pos[g * ROWS:(g + 1) * ROWS]


def run_gather(tokens, positions, embed_table, pos_table, time):
    vm = pl.BlockSpec(memory_space=pltpu.VMEM)
    hbm = pl.BlockSpec(memory_space=pltpu.HBM)
    d_model = embed_table.shape[1]
    rows = pltpu.VMEM((2, ROWS, d_model), BF16)
    return pl.pallas_call(
        gather_kernel,
        out_shape=(rows, rows, pltpu.VMEM((2, HEADS * ROWS, time), jnp.int32)),
        in_specs=[hbm] * 4,
        out_specs=(vm, vm, vm),
        scratch_shapes=[pltpu.VMEM((8 * BATCH, d_model), BF16), pltpu.VMEM((8 * BATCH, d_model), BF16),
                        pltpu.SMEM((BATCH,), jnp.int32), pltpu.SMEM((BATCH,), jnp.int32),
                        pltpu.SemaphoreType.DMA((2, BATCH)), pltpu.SemaphoreType.DMA((2,))],
        compiler_params=pltpu.CompilerParams(vmem_limit_bytes=GATHER_VMEM),
        name='gather_rows',
    )(*in_hbm(tokens, positions, embed_table, pos_table))


N_TILES = 3


def final_kernel(h_ref, table_ref, sk_ref, sv_ref, logits_ref, sk_out, sv_out, sems):
    copies = [pltpu.make_async_copy(sk_ref, sk_out, sems.at[0]), pltpu.make_async_copy(sv_ref, sv_out, sems.at[1])]
    for c in copies:
        c.start()
    h_t = h_ref[...].astype(F32).T.astype(BF16)
    tile = table_ref.shape[0] // N_TILES
    for i in range(N_TILES):
        logits_ref[:, i * tile:(i + 1) * tile] = dot(table_ref[i * tile:(i + 1) * tile], h_t).T
    for c in copies:
        c.wait()


def run_final(hidden, table, sk, sv):
    vm = pl.BlockSpec(memory_space=pltpu.VMEM)
    hbm = pl.BlockSpec(memory_space=pltpu.HBM)
    cache = jax.ShapeDtypeStruct(sk.shape, BF16)
    return pl.pallas_call(
        final_kernel,
        out_shape=(jax.ShapeDtypeStruct((BATCH, table.shape[0]), F32), cache, cache),
        in_specs=[vm] * 4,
        out_specs=(vm, hbm, hbm),
        scratch_shapes=[pltpu.SemaphoreType.DMA((2,))],
        compiler_params=pltpu.CompilerParams(vmem_limit_bytes=FINAL_VMEM),
        name='logits_and_caches',
    )(hidden, table, sk, sv)


def solution(mesh):
    def local_step(tokens, positions, self_keys, self_vals, cross_keys, cross_vals, embed_table, pos_table, w_qkv, w_cq, in_bias, w_out, out_bias, w_fc1, b_fc1, w_fc2, ln_layers, ln_final):
        d_model = embed_table.shape[1]

        def rows_by_time(cache):
            return jnp.transpose(cache, (0, 1, 3, 4, 2)).reshape(LAYERS, BATCH * HD, cache.shape[2])

        def as_cache(rows):
            return jnp.transpose(rows.reshape(LAYERS, BATCH, HEADS, HEAD_DIM, rows.shape[2]), (0, 1, 4, 2, 3))

        sk, sv = rows_by_time(self_keys), rows_by_time(self_vals)
        emb, pos, posn = run_gather(tokens, positions, embed_table, pos_table, sk.shape[2])
        hidden, table, sk, sv = run_core(
            emb, pos, posn, in_bias, jnp.transpose(out_bias, (1, 0, 2)), b_fc1, ln_layers.reshape(-1, 2, d_model), ln_final[None],
            embed_table, sk, sv, rows_by_time(cross_keys), rows_by_time(cross_vals),
            jnp.transpose(w_qkv, (0, 2, 3, 4, 1)).reshape(LAYERS, 3 * HD, d_model),
            jnp.transpose(w_cq, (0, 2, 3, 1)).reshape(LAYERS, HD, d_model),
            w_out.reshape(LAYERS, 2, HD, d_model), w_fc1, w_fc2)
        logits, new_sk, new_sv = run_final(hidden, table, sk, sv)
        return logits, as_cache(new_sk), as_cache(new_sv)

    batch_spec = P('dp')
    cache_spec = P(None, 'dp', None, 'tp', None)
    in_specs = (batch_spec, batch_spec, cache_spec, cache_spec, cache_spec, cache_spec, P('tp', None), P(None, None), P(None, None, None, 'tp', None), P(None, None, 'tp', None), P(None, None, 'tp', None), P(None, None, 'tp', None, None), P(None, None, None), P(None, None, 'tp'), P(None, 'tp'), P(None, 'tp', None), P(None, None, None, None), P(None, None))
    out_specs = (P('dp', 'tp'), cache_spec, cache_spec)
    return jax.shard_map(local_step, mesh=mesh, in_specs=in_specs, out_specs=out_specs, check_vma=False)
```

```python
import functools

import jax
import jax.numpy as jnp
from jax import lax
from jax.experimental import pallas as pl
from jax.experimental.pallas import tpu as pltpu
from jax.sharding import PartitionSpec as P

BF16 = jnp.bfloat16
F32 = jnp.float32
MESH = pl.DeviceIdType.MESH
N_TP = 8
OWNERS = (3, 5)
NEAR_FIRST = (2, 1, 0, 5, 4, 7, 6)
ODD_FIRST = (1, 5, 7)
ROWS = 8
BATCH = 16
HEADS = 2
HEAD_DIM = 64
HD = HEADS * HEAD_DIM
LAYERS = 2
GROUP_ROWS = 8 * 128
N_PHASES = 1 + 3 * LAYERS
CORE_VMEM = 32 << 20
GATHER_VMEM = 4 << 20
FINAL_VMEM = 6 << 20
NEG = -1e30


def dot(a, b):
    return jnp.dot(a, b, preferred_element_type=F32)


def dot_nt(a, b):
    return lax.dot_general(a, b, (((1,), (1,)), ((), ())), preferred_element_type=F32)


def in_hbm(*arrays):
    return tuple(pltpu.with_memory_space_constraint(a, pltpu.HBM) for a in arrays)


def layer_norm(x, gain, shift):
    mean = jnp.mean(x, axis=-1, keepdims=True)
    centred = x - mean
    var = jnp.mean(centred * centred, axis=-1, keepdims=True)
    return (centred * lax.rsqrt(var + 1e-5) * gain + shift).astype(BF16)


def head_row(ref, *idx):
    v = ref[idx]
    return jnp.concatenate([v[0:1], v[1:2]], axis=1)


def spread_queries(q):
    q2 = jnp.concatenate([q, q], axis=0)
    row = lax.broadcasted_iota(jnp.int32, q2.shape, 0)
    lane = lax.broadcasted_iota(jnp.int32, q2.shape, 1)
    q2 = jnp.where((row // ROWS) == (lane // HEAD_DIM), q2, 0.0)
    rb = row % ROWS
    return jnp.concatenate([jnp.where(rb == b, q2, 0.0).astype(BF16) for b in range(ROWS)], axis=1)


def gather_heads(mixed):
    row = lax.broadcasted_iota(jnp.int32, (HEADS * ROWS, HD), 0) % ROWS
    acc = jnp.zeros(row.shape, F32)
    for b in range(ROWS):
        acc = jnp.where(row == b, mixed[:, b * HD:(b + 1) * HD], acc)
    lane = lax.broadcasted_iota(jnp.int32, (ROWS, HD), 1)
    return jnp.where(lane < HEAD_DIM, acc[:ROWS], acc[ROWS:])


def core_kernel(emb_ref, pos_ref, posn_ref, in_bias_hbm, out_bias_hbm, b_fc1_hbm, ln_hbm, lnf_hbm,
                table_hbm, sk_hbm, sv_hbm, ck_hbm, cv_hbm, wqkv_hbm, wcq_hbm, wout_hbm, wfc1_hbm, wfc2_hbm,
                h_out, table, sk, sv,
                ck, cv, wqkv, wcq, wout, wfc1, wfc2, pair_fc1, pair_fc2, pair_b,
                in_bias_ref, out_bias_ref, b_fc1_ref, ln_ref,
                emb_rs, part_send, part_rs, hbuf, x_ref, new_ref,
                small_sems, load_sems, half_sems, pair_send, pair_recv, rs_send, rs_recv, ag_send, ag_recv):
    me = lax.axis_index('tp')
    n_ln = ln_hbm.shape[0]
    smalls = [(in_bias_hbm, in_bias_ref), (out_bias_hbm, out_bias_ref), (b_fc1_hbm, b_fc1_ref),
              (ln_hbm, ln_ref.at[pl.ds(0, n_ln)]), (lnf_hbm, ln_ref.at[pl.ds(n_ln, 1)])]
    small_loads = [pltpu.make_async_copy(src, dst, small_sems.at[i]) for i, (src, dst) in enumerate(smalls)]
    table_load = pltpu.make_async_copy(table_hbm, table, small_sems.at[len(smalls)])
    refs = {'wqkv': (wqkv_hbm, wqkv), 'sk': (sk_hbm, sk), 'sv': (sv_hbm, sv), 'wout': (wout_hbm, wout),
            'wcq': (wcq_hbm, wcq), 'fc1': (wfc1_hbm, wfc1), 'fc2': (wfc2_hbm, wfc2)}

    def load(name, l):
        src, dst = refs[name]
        return pltpu.make_async_copy(src.at[l], dst.at[l], load_sems.at[list(refs).index(name), l])

    def rows_of(g):
        return pl.ds(pl.multiple_of(g * GROUP_ROWS, GROUP_ROWS), GROUP_ROWS)

    def load_half(i, l, g):
        src, dst = ((ck_hbm, ck), (cv_hbm, cv))[i]
        return pltpu.make_async_copy(src.at[l, rows_of(g)], dst.at[rows_of(g)], half_sems.at[i, g])

    for c in small_loads:
        c.start()
    for name in ('wqkv', 'sk', 'sv', 'wout', 'wcq'):
        load(name, 0).start()
    for g in range(2):
        for i in range(2):
            load_half(i, 0, g).start()
    odd = me % 2 == 1

    @pl.when(odd)
    def _():
        for name in ('fc1', 'fc2'):
            load(name, 0).start()

    barrier = pltpu.get_barrier_semaphore()
    is_owner = (me == OWNERS[0]) | (me == OWNERS[1])
    for d in range(N_TP):
        @pl.when((me != d) if d in OWNERS else is_owner)
        def _():
            pl.semaphore_signal(barrier, inc=1, device_id={'tp': d}, device_id_type=MESH)

    @pl.when(odd & jnp.logical_not(is_owner))
    def _():
        pl.semaphore_signal(barrier, inc=1, device_id={'tp': me - 1}, device_id_type=MESH)

    @pl.when(is_owner)
    def _():
        pl.semaphore_wait(barrier, N_TP - 1)

    @pl.when(odd & jnp.logical_not(is_owner))
    def _():
        pl.semaphore_wait(barrier, 2)

    alone = jnp.logical_not(odd) & (me != OWNERS[0] - 1) & (me != OWNERS[1] - 1)

    @pl.when(alone)
    def _():
        pl.semaphore_wait(barrier, 3)

    @pl.when(jnp.logical_not(odd) & jnp.logical_not(alone))
    def _():
        pl.semaphore_wait(barrier, 2)

    def owner_of(g):
        return OWNERS[0] + (OWNERS[1] - OWNERS[0]) * g

    def others(g, of=NEAR_FIRST):
        return [d + g * (N_TP - 2 - 2 * (d // 2) + d % 2 - d) for d in of]

    def rs_copy(ph, g, i):
        if isinstance(ph, int) and ph == 0:
            src, dst = emb_ref.at[g], emb_rs.at[i]
        else:
            src, dst = part_send.at[ph - 1, g], part_rs.at[ph - 1, i]
        return pltpu.make_async_remote_copy(src_ref=src, dst_ref=dst, send_sem=rs_send.at[ph, g], recv_sem=rs_recv.at[ph, i],
                                            device_id={'tp': owner_of(g)}, device_id_type=MESH)

    def ag_copy(ph, g, d):
        return pltpu.make_async_remote_copy(src_ref=hbuf.at[ph, g], dst_ref=hbuf.at[ph, g], send_sem=ag_send.at[ph, d], recv_sem=ag_recv.at[ph, g],
                                            device_id={'tp': d}, device_id_type=MESH)

    def send(ph, g):
        @pl.when(me != owner_of(g))
        def _():
            rs_copy(ph, g, me).start()

    my_group = (me - OWNERS[0]) // (OWNERS[1] - OWNERS[0])

    def reduce(ph, bias, summed=NEAR_FIRST, told=NEAR_FIRST):
        @pl.when(is_owner)
        def _():
            g = my_group
            first = bias is None
            total = (emb_ref[g] if first else part_send[ph - 1, g]).astype(F32)
            base = pos_ref[g].astype(F32) if first else x_ref[...] + bias
            for i in others(g, summed):
                rs_copy(ph, g, i).wait_recv()
                total = total + (emb_rs[i] if first else part_rs[ph - 1, i]).astype(F32)
            x = total.astype(BF16).astype(F32) + base
            x_ref[...] = x
            hbuf[ph, g] = layer_norm(x, ln_ref[ph, 0:1], ln_ref[ph, 1:2])
            for d in reversed(others(g, told)):
                ag_copy(ph, g, d).start()

    pairs = [pltpu.make_async_remote_copy(src_ref=src, dst_ref=dst, send_sem=pair_send.at[i], recv_sem=pair_recv.at[i],
                                          device_id={'tp': jnp.minimum(me + 1, N_TP - 1)}, device_id_type=MESH)
             for i, (src, dst) in enumerate([(wfc1_hbm.at[0], pair_fc1.at[0]), (wfc2_hbm.at[0], pair_fc2.at[0]), (b_fc1_hbm, pair_b),
                                             (wfc1_hbm.at[1], pair_fc1.at[1]), (wfc2_hbm.at[1], pair_fc2.at[1])])]

    def receive(ph, g):
        @pl.when(me != owner_of(g))
        def _():
            ag_copy(ph, g, 0).wait_recv()
        return hbuf[ph, g]

    for g in range(2):
        send(0, g)

    @pl.when(jnp.logical_not(odd))
    def _():
        for c in pairs:
            c.start()

    for c in small_loads:
        c.wait()
    reduce(0, None)

    time = sk.shape[2]
    qk_scale = HEAD_DIM ** -0.5

    def attend_self(l, g, hidden):
        qkv = dot_nt(hidden, wqkv[l])
        q = (qkv[:, :HD] + head_row(in_bias_ref, l, 0)).astype(BF16).astype(F32)
        k_new = qkv[:, HD:2 * HD].astype(BF16).astype(F32)
        v_new = (qkv[:, 2 * HD:] + head_row(in_bias_ref, l, 1)).astype(BF16).astype(F32)
        new_ref[0, g] = k_new
        new_ref[1, g] = v_new
        prod = q * k_new
        s_new = jnp.concatenate([jnp.sum(prod[:, :HEAD_DIM], axis=1, keepdims=True), jnp.sum(prod[:, HEAD_DIM:], axis=1, keepdims=True)], axis=0)
        posn = posn_ref[g]
        t_idx = lax.broadcasted_iota(jnp.int32, posn.shape, 1)
        here = t_idx == posn
        s = jnp.where(here, s_new, dot(spread_queries(q), sk[l, rows_of(g)])) * qk_scale
        s = jnp.where(t_idx <= posn, s, NEG)
        e = jnp.exp(s - jnp.max(s, axis=-1, keepdims=True))
        w = (e / jnp.sum(e, axis=-1, keepdims=True)).astype(BF16).astype(F32)
        w_new = jnp.sum(jnp.where(here, w, 0.0), axis=-1, keepdims=True)
        w_old = jnp.where(here, 0.0, w)
        mixed = gather_heads(dot_nt(w_old.astype(BF16), sv[l, rows_of(g)]))
        lane = lax.broadcasted_iota(jnp.int32, (ROWS, HD), 1)
        w_row = jnp.where(lane < HEAD_DIM, w_new[:ROWS], w_new[ROWS:])
        o = (mixed + w_row * v_new).astype(BF16)
        return dot(o, wout[l, 0])

    def write_new(l, g):
        t_row = lax.broadcasted_iota(jnp.int32, (HD, time), 1)
        cols = [new_ref[i, g].T for i in range(2)]
        for b in range(ROWS):
            at = t_row == posn_ref[g, b:b + 1]
            rows = pl.ds(pl.multiple_of(g * GROUP_ROWS + b * HD, HD), HD)
            for ref, col in zip((sk, sv), cols):
                ref[l, rows] = jnp.where(at, col[:, b:b + 1], ref[l, rows].astype(F32)).astype(BF16)

    def attend_cross(l, g, hidden):
        q = (dot_nt(hidden, wcq[l]) + head_row(in_bias_ref, l, 2)).astype(BF16).astype(F32)
        load_half(0, l, g).wait()
        s = dot(spread_queries(q), ck[rows_of(g)]) * qk_scale
        e = jnp.exp(s - jnp.max(s, axis=-1, keepdims=True))
        w = e / jnp.sum(e, axis=-1, keepdims=True)
        load_half(1, l, g).wait()
        o = gather_heads(dot_nt(w.astype(BF16), cv[rows_of(g)])).astype(BF16)
        return dot(o, wout[l, 1])

    def mlp(l, g, hidden):
        part = None
        for fc1, b, fc2 in ((wfc1, b_fc1_ref, wfc2), (pair_fc1, pair_b, pair_fc2)):
            f = dot(hidden, fc1[l]) + b[pl.ds(l, 1)]
            act = (f * 0.5 * (1.0 + lax.erf(f * (2.0 ** -0.5)))).astype(BF16)
            half = dot(act, fc2[l])
            part = half if part is None else part + half
        return part

    def both_streams(body):
        lax.fori_loop(0, 2, lambda g, c: (body(g), c)[1], 0)

    def layer(l, carry):
        ph = 3 * l + 1

        def block(ph, compute, after=None):
            def stream(g):
                part_send[ph - 1, g] = compute(l, g, receive(ph - 1, g))
                send(ph, g)
                if after is not None:
                    after(g)
            both_streams(stream)

        for name in ('wqkv', 'sk', 'sv', 'wout'):
            load(name, l).wait()
        block(ph, attend_self)
        reduce(ph, out_bias_ref[0, pl.ds(l, 1)])

        @pl.when(l == 0)
        def _():
            for name in ('wqkv', 'sk', 'sv', 'wout', 'wcq'):
                load(name, 1).start()
            table_load.start()

            @pl.when(odd)
            def _():
                for name in ('fc1', 'fc2'):
                    load(name, 1).start()

        both_streams(lambda g: write_new(l, g))
        load('wcq', l).wait()

        def next_half(g):
            @pl.when(l + 1 < LAYERS)
            def _():
                for i in range(2):
                    load_half(i, l + 1, g).start()

        block(ph + 1, attend_cross, next_half)
        reduce(ph + 1, out_bias_ref[1, pl.ds(l, 1)], told=ODD_FIRST)

        @pl.when(odd)
        def _():
            load('fc1', l).wait()
            load('fc2', l).wait()

            @pl.when(l == 0)
            def _():
                for c in pairs:
                    c.wait_recv()

            block(ph + 2, mlp)

        reduce(ph + 2, out_bias_ref[2, pl.ds(l, 1)], summed=ODD_FIRST)
        return carry

    lax.fori_loop(0, LAYERS, layer, 0)

    def drain(ph, mlp_in=False, mlp_out=False):
        for g in range(2):
            @pl.when((me != OWNERS[g]) & (odd if mlp_out else True))
            def _():
                rs_copy(ph, g, me).wait_send()

        @pl.when(is_owner)
        def _():
            for d in others(my_group, ODD_FIRST if mlp_in else NEAR_FIRST):
                ag_copy(ph, my_group, d).wait_send()

    @pl.when(jnp.logical_not(odd))
    def _():
        for c in pairs:
            c.wait_send()

    drain(0)

    def drain_layer(l, carry):
        drain(3 * l + 1)
        drain(3 * l + 2, mlp_in=True)
        return carry

    lax.fori_loop(0, LAYERS, drain_layer, 0)
    last = N_PHASES - 1
    for ph in range(3, last, 3):
        drain(ph, mlp_out=True)
    table_load.wait()
    h_out[...] = jnp.concatenate([receive(last, 0), receive(last, 1)], axis=0)
    drain(last, mlp_out=True)


def run_core(emb, pos, posn, in_bias, out_bias, b_fc1, ln_layers, ln_final, table, sk, sv, ck, cv, wqkv, wcq, wout, wfc1, wfc2):
    vm = pl.BlockSpec(memory_space=pltpu.VMEM)
    hbm = pl.BlockSpec(memory_space=pltpu.HBM)
    d_model = emb.shape[-1]
    ln_rows = ln_layers.shape[0] + 1
    return pl.pallas_call(
        core_kernel,
        out_shape=(pltpu.VMEM((BATCH, d_model), BF16),) + tuple(pltpu.VMEM(a.shape, BF16) for a in (table, sk, sv)),
        in_specs=[vm] * 3 + [hbm] * 15,
        out_specs=(vm,) * 4,
        scratch_shapes=[pltpu.VMEM(a.shape[1:], BF16) for a in (ck, cv)]
        + [pltpu.VMEM(a.shape, BF16) for a in (wqkv, wcq, wout, wfc1, wfc2, wfc1, wfc2)]
        + [pltpu.VMEM(b_fc1.shape, F32)]
        + [pltpu.VMEM(a.shape, F32) for a in (in_bias, out_bias, b_fc1)]
        + [pltpu.VMEM((ln_rows, 2, d_model), F32),
           pltpu.VMEM((N_TP, ROWS, d_model), BF16),
           pltpu.VMEM((N_PHASES - 1, 2, ROWS, d_model), F32),
           pltpu.VMEM((N_PHASES - 1, N_TP, ROWS, d_model), F32),
           pltpu.VMEM((N_PHASES, 2, ROWS, d_model), BF16),
           pltpu.VMEM((ROWS, d_model), F32),
           pltpu.VMEM((2, 2, ROWS, HD), F32),
           pltpu.SemaphoreType.DMA((6,)),
           pltpu.SemaphoreType.DMA((7, LAYERS)),
           pltpu.SemaphoreType.DMA((2, 2)),
           pltpu.SemaphoreType.DMA((5,)),
           pltpu.SemaphoreType.DMA((5,)),
           pltpu.SemaphoreType.DMA((N_PHASES, 2)),
           pltpu.SemaphoreType.DMA((N_PHASES, N_TP)),
           pltpu.SemaphoreType.DMA((N_PHASES, N_TP)),
           pltpu.SemaphoreType.DMA((N_PHASES, 2))],
        compiler_params=pltpu.CompilerParams(collective_id=0, has_side_effects=True, vmem_limit_bytes=CORE_VMEM),
        cost_estimate=pl.CostEstimate(flops=4 << 30, bytes_accessed=150 << 20, transcendentals=0),
        name='decode_layers',
    )(emb, pos, posn, *in_hbm(in_bias, out_bias, b_fc1, ln_layers, ln_final, table, sk, sv, ck, cv, wqkv, wcq, wout, wfc1, wfc2))


def gather_kernel(tok_hbm, posn_hbm, table_hbm, pos_hbm, emb_out, pos_out, posn_out, emb_buf, pos_buf, tok_ref, pos_ref, sems, idx_sems):
    idx = [pltpu.make_async_copy(tok_hbm, tok_ref, idx_sems.at[0]), pltpu.make_async_copy(posn_hbm, pos_ref, idx_sems.at[1])]
    for c in idx:
        c.start()
    for c in idx:
        c.wait()
    shard_rows = table_hbm.shape[0]
    base = lax.axis_index('tp') * shard_rows
    copies = []
    for b in range(BATCH):
        row = jnp.clip(tok_ref[b] - base, 0, shard_rows - 1)
        at = pl.multiple_of((row // 8) * 8, 8)
        copies.append(pltpu.make_async_copy(table_hbm.at[pl.ds(at, 8)], emb_buf.at[pl.ds(b * 8, 8)], sems.at[0, b]))
        at = pl.multiple_of((pos_ref[b] // 8) * 8, 8)
        copies.append(pltpu.make_async_copy(pos_hbm.at[pl.ds(at, 8)], pos_buf.at[pl.ds(b * 8, 8)], sems.at[1, b]))
    for c in copies:
        c.start()
    row_i = lax.broadcasted_iota(jnp.int32, (BATCH, 8 * BATCH), 0)
    lane_i = lax.broadcasted_iota(jnp.int32, (BATCH, 8 * BATCH), 1)
    tok_at = jnp.zeros((BATCH, 8 * BATCH), jnp.int32)
    pos_at = jnp.zeros((BATCH, 8 * BATCH), jnp.int32)
    posn_row = lax.broadcasted_iota(jnp.int32, (BATCH, posn_out.shape[2]), 0)
    posn = jnp.zeros(posn_row.shape, jnp.int32)
    for b in range(BATCH):
        row = tok_ref[b] - base
        owned = (row >= 0) & (row < shard_rows)
        tok_at = jnp.where(row_i == b, jnp.where(owned, b * 8 + row % 8, -1), tok_at)
        pos_at = jnp.where(row_i == b, b * 8 + pos_ref[b] % 8, pos_at)
        posn = jnp.where(posn_row == b, pos_ref[b], posn)
    for g in range(2):
        posn_out[g] = jnp.concatenate([posn[g * ROWS:(g + 1) * ROWS]] * HEADS, axis=0)
    pick_tok = jnp.where(lane_i == tok_at, 1.0, 0.0).astype(BF16)
    pick_pos = jnp.where(lane_i == pos_at, 1.0, 0.0).astype(BF16)
    for c in copies:
        c.wait()
    emb = dot(pick_tok, emb_buf[...]).astype(BF16)
    pos = dot(pick_pos, pos_buf[...]).astype(BF16)
    for g in range(2):
        emb_out[g] = emb[g * ROWS:(g + 1) * ROWS]
        pos_out[g] = pos[g * ROWS:(g + 1) * ROWS]


def run_gather(tokens, positions, embed_table, pos_table, time):
    vm = pl.BlockSpec(memory_space=pltpu.VMEM)
    hbm = pl.BlockSpec(memory_space=pltpu.HBM)
    d_model = embed_table.shape[1]
    rows = pltpu.VMEM((2, ROWS, d_model), BF16)
    return pl.pallas_call(
        gather_kernel,
        out_shape=(rows, rows, pltpu.VMEM((2, HEADS * ROWS, time), jnp.int32)),
        in_specs=[hbm] * 4,
        out_specs=(vm, vm, vm),
        scratch_shapes=[pltpu.VMEM((8 * BATCH, d_model), BF16), pltpu.VMEM((8 * BATCH, d_model), BF16),
                        pltpu.SMEM((BATCH,), jnp.int32), pltpu.SMEM((BATCH,), jnp.int32),
                        pltpu.SemaphoreType.DMA((2, BATCH)), pltpu.SemaphoreType.DMA((2,))],
        compiler_params=pltpu.CompilerParams(vmem_limit_bytes=GATHER_VMEM),
        name='gather_rows',
    )(*in_hbm(tokens, positions, embed_table, pos_table))


N_TILES = 3


def final_kernel(h_ref, table_ref, sk_ref, sv_ref, logits_ref, sk_out, sv_out, sems):
    copies = [pltpu.make_async_copy(sk_ref, sk_out, sems.at[0]), pltpu.make_async_copy(sv_ref, sv_out, sems.at[1])]
    for c in copies:
        c.start()
    h_t = h_ref[...].astype(F32).T.astype(BF16)
    tile = table_ref.shape[0] // N_TILES
    for i in range(N_TILES):
        logits_ref[:, i * tile:(i + 1) * tile] = dot(table_ref[i * tile:(i + 1) * tile], h_t).T
    for c in copies:
        c.wait()


def run_final(hidden, table, sk, sv):
    vm = pl.BlockSpec(memory_space=pltpu.VMEM)
    hbm = pl.BlockSpec(memory_space=pltpu.HBM)
    cache = jax.ShapeDtypeStruct(sk.shape, BF16)
    return pl.pallas_call(
        final_kernel,
        out_shape=(jax.ShapeDtypeStruct((BATCH, table.shape[0]), F32), cache, cache),
        in_specs=[vm] * 4,
        out_specs=(vm, hbm, hbm),
        scratch_shapes=[pltpu.SemaphoreType.DMA((2,))],
        compiler_params=pltpu.CompilerParams(vmem_limit_bytes=FINAL_VMEM),
        name='logits_and_caches',
    )(hidden, table, sk, sv)


def solution(mesh):
    def local_step(tokens, positions, self_keys, self_vals, cross_keys, cross_vals, embed_table, pos_table, w_qkv, w_cq, in_bias, w_out, out_bias, w_fc1, b_fc1, w_fc2, ln_layers, ln_final):
        d_model = embed_table.shape[1]

        def rows_by_time(cache):
            return jnp.transpose(cache, (0, 1, 3, 4, 2)).reshape(LAYERS, BATCH * HD, cache.shape[2])

        def as_cache(rows):
            return jnp.transpose(rows.reshape(LAYERS, BATCH, HEADS, HEAD_DIM, rows.shape[2]), (0, 1, 4, 2, 3))

        sk, sv = rows_by_time(self_keys), rows_by_time(self_vals)
        emb, pos, posn = run_gather(tokens, positions, embed_table, pos_table, sk.shape[2])
        hidden, table, sk, sv = run_core(
            emb, pos, posn, in_bias, jnp.transpose(out_bias, (1, 0, 2)), b_fc1, ln_layers.reshape(-1, 2, d_model), ln_final[None],
            embed_table, sk, sv, rows_by_time(cross_keys), rows_by_time(cross_vals),
            jnp.transpose(w_qkv, (0, 2, 3, 4, 1)).reshape(LAYERS, 3 * HD, d_model),
            jnp.transpose(w_cq, (0, 2, 3, 1)).reshape(LAYERS, HD, d_model),
            w_out.reshape(LAYERS, 2, HD, d_model), w_fc1, w_fc2)
        logits, new_sk, new_sv = run_final(hidden, table, sk, sv)
        return logits, as_cache(new_sk), as_cache(new_sv)

    batch_spec = P('dp')
    cache_spec = P(None, 'dp', None, 'tp', None)
    in_specs = (batch_spec, batch_spec, cache_spec, cache_spec, cache_spec, cache_spec, P('tp', None), P(None, None), P(None, None, None, 'tp', None), P(None, None, 'tp', None), P(None, None, 'tp', None), P(None, None, 'tp', None, None), P(None, None, None), P(None, None, 'tp'), P(None, 'tp'), P(None, 'tp', None), P(None, None, None, None), P(None, None))
    out_specs = (P('dp', 'tp'), cache_spec, cache_spec)
    return jax.shard_map(local_step, mesh=mesh, in_specs=in_specs, out_specs=out_specs, check_vma=False)
```

```python
import functools

import jax
import jax.numpy as jnp
from jax import lax
from jax.experimental import pallas as pl
from jax.experimental.pallas import tpu as pltpu
from jax.sharding import PartitionSpec as P

BF16 = jnp.bfloat16
F32 = jnp.float32
MESH = pl.DeviceIdType.MESH
N_TP = 8
OWNERS = (3, 5)
NEAR_FIRST = (2, 1, 0, 5, 4, 7, 6)
ODD_FIRST = (1, 5, 7)
ROWS = 8
BATCH = 16
HEADS = 2
HEAD_DIM = 64
HD = HEADS * HEAD_DIM
LAYERS = 2
GROUP_ROWS = 8 * 128
N_PHASES = 1 + 3 * LAYERS
CORE_VMEM = 32 << 20
GATHER_VMEM = 4 << 20
FINAL_VMEM = 6 << 20
NEG = -1e30


def dot(a, b):
    return jnp.dot(a, b, preferred_element_type=F32)


def dot_nt(a, b):
    return lax.dot_general(a, b, (((1,), (1,)), ((), ())), preferred_element_type=F32)


def in_hbm(*arrays):
    return tuple(pltpu.with_memory_space_constraint(a, pltpu.HBM) for a in arrays)


def layer_norm(x, gain, shift):
    mean = jnp.mean(x, axis=-1, keepdims=True)
    centred = x - mean
    var = jnp.mean(centred * centred, axis=-1, keepdims=True)
    return (centred * lax.rsqrt(var + 1e-5) * gain + shift).astype(BF16)


def head_row(ref, *idx):
    v = ref[idx]
    return jnp.concatenate([v[0:1], v[1:2]], axis=1)


def spread_queries(q):
    q2 = jnp.concatenate([q, q], axis=0)
    row = lax.broadcasted_iota(jnp.int32, q2.shape, 0)
    lane = lax.broadcasted_iota(jnp.int32, q2.shape, 1)
    q2 = jnp.where((row // ROWS) == (lane // HEAD_DIM), q2, 0.0)
    rb = row % ROWS
    return jnp.concatenate([jnp.where(rb == b, q2, 0.0).astype(BF16) for b in range(ROWS)], axis=1)


def gather_heads(mixed):
    row = lax.broadcasted_iota(jnp.int32, (HEADS * ROWS, HD), 0) % ROWS
    acc = jnp.zeros(row.shape, F32)
    for b in range(ROWS):
        acc = jnp.where(row == b, mixed[:, b * HD:(b + 1) * HD], acc)
    lane = lax.broadcasted_iota(jnp.int32, (ROWS, HD), 1)
    return jnp.where(lane < HEAD_DIM, acc[:ROWS], acc[ROWS:])


def core_kernel(emb_ref, pos_ref, posn_ref, in_bias_hbm, out_bias_hbm, b_fc1_hbm, ln_hbm, lnf_hbm,
                table_hbm, sk_hbm, sv_hbm, ck_hbm, cv_hbm, wqkv_hbm, wcq_hbm, wout_hbm, wfc1_hbm, wfc2_hbm,
                h_out, table, sk, sv,
                ck, cv, wqkv, wcq, wout, wfc1, wfc2, pair_fc1, pair_fc2, pair_b,
                in_bias_ref, out_bias_ref, b_fc1_ref, ln_ref,
                emb_rs, part_send, part_rs, hbuf, x_ref, new_ref,
                small_sems, load_sems, half_sems, pair_send, pair_recv, rs_send, rs_recv, ag_send, ag_recv):
    me = lax.axis_index('tp')
    n_ln = ln_hbm.shape[0]
    smalls = [(in_bias_hbm, in_bias_ref), (out_bias_hbm, out_bias_ref), (b_fc1_hbm, b_fc1_ref),
              (ln_hbm, ln_ref.at[pl.ds(0, n_ln)]), (lnf_hbm, ln_ref.at[pl.ds(n_ln, 1)])]
    small_loads = [pltpu.make_async_copy(src, dst, small_sems.at[i]) for i, (src, dst) in enumerate(smalls)]
    table_load = pltpu.make_async_copy(table_hbm, table, small_sems.at[len(smalls)])
    refs = {'wqkv': (wqkv_hbm, wqkv), 'sk': (sk_hbm, sk), 'sv': (sv_hbm, sv), 'wout': (wout_hbm, wout),
            'wcq': (wcq_hbm, wcq), 'fc1': (wfc1_hbm, wfc1), 'fc2': (wfc2_hbm, wfc2)}

    def load(name, l):
        src, dst = refs[name]
        return pltpu.make_async_copy(src.at[l], dst.at[l], load_sems.at[list(refs).index(name), l])

    def rows_of(g):
        return pl.ds(pl.multiple_of(g * GROUP_ROWS, GROUP_ROWS), GROUP_ROWS)

    def load_half(i, l, g):
        src, dst = ((ck_hbm, ck), (cv_hbm, cv))[i]
        return pltpu.make_async_copy(src.at[l, rows_of(g)], dst.at[rows_of(g)], half_sems.at[i, g])

    for c in small_loads:
        c.start()
    odd = me % 2 == 1

    barrier = pltpu.get_barrier_semaphore()
    is_owner = (me == OWNERS[0]) | (me == OWNERS[1])
    for d in range(N_TP):
        @pl.when((me != d) if d in OWNERS else is_owner)
        def _():
            pl.semaphore_signal(barrier, inc=1, device_id={'tp': d}, device_id_type=MESH)

    @pl.when(odd & jnp.logical_not(is_owner))
    def _():
        pl.semaphore_signal(barrier, inc=1, device_id={'tp': me - 1}, device_id_type=MESH)

    @pl.when(is_owner)
    def _():
        pl.semaphore_wait(barrier, N_TP - 1)

    @pl.when(odd & jnp.logical_not(is_owner))
    def _():
        pl.semaphore_wait(barrier, 2)

    alone = jnp.logical_not(odd) & (me != OWNERS[0] - 1) & (me != OWNERS[1] - 1)

    @pl.when(alone)
    def _():
        pl.semaphore_wait(barrier, 3)

    @pl.when(jnp.logical_not(odd) & jnp.logical_not(alone))
    def _():
        pl.semaphore_wait(barrier, 2)

    def owner_of(g):
        return OWNERS[0] + (OWNERS[1] - OWNERS[0]) * g

    def others(g, of=NEAR_FIRST):
        return [d + g * (N_TP - 2 - 2 * (d // 2) + d % 2 - d) for d in of]

    def rs_copy(ph, g, i):
        if isinstance(ph, int) and ph == 0:
            src, dst = emb_ref.at[g], emb_rs.at[i]
        else:
            src, dst = part_send.at[ph - 1, g], part_rs.at[ph - 1, i]
        return pltpu.make_async_remote_copy(src_ref=src, dst_ref=dst, send_sem=rs_send.at[ph, g], recv_sem=rs_recv.at[ph, i],
                                            device_id={'tp': owner_of(g)}, device_id_type=MESH)

    def ag_copy(ph, g, d):
        return pltpu.make_async_remote_copy(src_ref=hbuf.at[ph, g], dst_ref=hbuf.at[ph, g], send_sem=ag_send.at[ph, d], recv_sem=ag_recv.at[ph, g],
                                            device_id={'tp': d}, device_id_type=MESH)

    def send(ph, g):
        @pl.when(me != owner_of(g))
        def _():
            rs_copy(ph, g, me).start()

    my_group = (me - OWNERS[0]) // (OWNERS[1] - OWNERS[0])

    def reduce(ph, bias, summed=NEAR_FIRST, told=NEAR_FIRST):
        @pl.when(is_owner)
        def _():
            g = my_group
            first = bias is None
            total = (emb_ref[g] if first else part_send[ph - 1, g]).astype(F32)
            base = pos_ref[g].astype(F32) if first else x_ref[...] + bias
            for i in others(g, summed):
                rs_copy(ph, g, i).wait_recv()
                total = total + (emb_rs[i] if first else part_rs[ph - 1, i]).astype(F32)
            x = total.astype(BF16).astype(F32) + base
            x_ref[...] = x
            hbuf[ph, g] = layer_norm(x, ln_ref[ph, 0:1], ln_ref[ph, 1:2])
            for d in reversed(others(g, told)):
                ag_copy(ph, g, d).start()

    pairs = [pltpu.make_async_remote_copy(src_ref=src, dst_ref=dst, send_sem=pair_send.at[i], recv_sem=pair_recv.at[i],
                                          device_id={'tp': jnp.minimum(me + 1, N_TP - 1)}, device_id_type=MESH)
             for i, (src, dst) in enumerate([(wfc1_hbm.at[0], pair_fc1.at[0]), (wfc2_hbm.at[0], pair_fc2.at[0]), (b_fc1_hbm, pair_b),
                                             (wfc1_hbm.at[1], pair_fc1.at[1]), (wfc2_hbm.at[1], pair_fc2.at[1])])]

    def receive(ph, g):
        @pl.when(me != owner_of(g))
        def _():
            ag_copy(ph, g, 0).wait_recv()
        return hbuf[ph, g]

    for g in range(2):
        send(0, g)

    @pl.when(jnp.logical_not(odd))
    def _():
        for c in pairs:
            c.start()

    for name in ('wqkv', 'sk', 'sv', 'wout', 'wcq'):
        load(name, 0).start()
    for g in range(2):
        for i in range(2):
            load_half(i, 0, g).start()
    @pl.when(odd)
    def _():
        for name in ('fc1', 'fc2'):
            load(name, 0).start()

    for c in small_loads:
        c.wait()
    reduce(0, None)

    time = sk.shape[2]
    qk_scale = HEAD_DIM ** -0.5

    def attend_self(l, g, hidden):
        qkv = dot_nt(hidden, wqkv[l])
        q = (qkv[:, :HD] + head_row(in_bias_ref, l, 0)).astype(BF16).astype(F32)
        k_new = qkv[:, HD:2 * HD].astype(BF16).astype(F32)
        v_new = (qkv[:, 2 * HD:] + head_row(in_bias_ref, l, 1)).astype(BF16).astype(F32)
        new_ref[0, g] = k_new
        new_ref[1, g] = v_new
        prod = q * k_new
        s_new = jnp.concatenate([jnp.sum(prod[:, :HEAD_DIM], axis=1, keepdims=True), jnp.sum(prod[:, HEAD_DIM:], axis=1, keepdims=True)], axis=0)
        posn = posn_ref[g]
        t_idx = lax.broadcasted_iota(jnp.int32, posn.shape, 1)
        here = t_idx == posn
        s = jnp.where(here, s_new, dot(spread_queries(q), sk[l, rows_of(g)])) * qk_scale
        s = jnp.where(t_idx <= posn, s, NEG)
        e = jnp.exp(s - jnp.max(s, axis=-1, keepdims=True))
        w = (e / jnp.sum(e, axis=-1, keepdims=True)).astype(BF16).astype(F32)
        w_new = jnp.sum(jnp.where(here, w, 0.0), axis=-1, keepdims=True)
        w_old = jnp.where(here, 0.0, w)
        mixed = gather_heads(dot_nt(w_old.astype(BF16), sv[l, rows_of(g)]))
        lane = lax.broadcasted_iota(jnp.int32, (ROWS, HD), 1)
        w_row = jnp.where(lane < HEAD_DIM, w_new[:ROWS], w_new[ROWS:])
        o = (mixed + w_row * v_new).astype(BF16)
        return dot(o, wout[l, 0])

    def write_new(l, g):
        t_row = lax.broadcasted_iota(jnp.int32, (HD, time), 1)
        cols = [new_ref[i, g].T for i in range(2)]
        for b in range(ROWS):
            at = t_row == posn_ref[g, b:b + 1]
            rows = pl.ds(pl.multiple_of(g * GROUP_ROWS + b * HD, HD), HD)
            for ref, col in zip((sk, sv), cols):
                ref[l, rows] = jnp.where(at, col[:, b:b + 1], ref[l, rows].astype(F32)).astype(BF16)

    def attend_cross(l, g, hidden):
        q = (dot_nt(hidden, wcq[l]) + head_row(in_bias_ref, l, 2)).astype(BF16).astype(F32)
        load_half(0, l, g).wait()
        s = dot(spread_queries(q), ck[rows_of(g)]) * qk_scale
        e = jnp.exp(s - jnp.max(s, axis=-1, keepdims=True))
        w = e / jnp.sum(e, axis=-1, keepdims=True)
        load_half(1, l, g).wait()
        o = gather_heads(dot_nt(w.astype(BF16), cv[rows_of(g)])).astype(BF16)
        return dot(o, wout[l, 1])

    def mlp(l, g, hidden):
        part = None
        for fc1, b, fc2 in ((wfc1, b_fc1_ref, wfc2), (pair_fc1, pair_b, pair_fc2)):
            f = dot(hidden, fc1[l]) + b[pl.ds(l, 1)]
            act = (f * 0.5 * (1.0 + lax.erf(f * (2.0 ** -0.5)))).astype(BF16)
            half = dot(act, fc2[l])
            part = half if part is None else part + half
        return part

    def both_streams(body):
        lax.fori_loop(0, 2, lambda g, c: (body(g), c)[1], 0)

    def layer(l, carry):
        ph = 3 * l + 1

        def block(ph, compute, after=None):
            def stream(g):
                part_send[ph - 1, g] = compute(l, g, receive(ph - 1, g))
                send(ph, g)
                if after is not None:
                    after(g)
            both_streams(stream)

        for name in ('wqkv', 'sk', 'sv', 'wout'):
            load(name, l).wait()
        block(ph, attend_self)
        reduce(ph, out_bias_ref[0, pl.ds(l, 1)])

        @pl.when(l == 0)
        def _():
            for name in ('wqkv', 'sk', 'sv', 'wout', 'wcq'):
                load(name, 1).start()
            table_load.start()

            @pl.when(odd)
            def _():
                for name in ('fc1', 'fc2'):
                    load(name, 1).start()

        both_streams(lambda g: write_new(l, g))
        load('wcq', l).wait()

        def next_half(g):
            @pl.when(l + 1 < LAYERS)
            def _():
                for i in range(2):
                    load_half(i, l + 1, g).start()

        block(ph + 1, attend_cross, next_half)
        reduce(ph + 1, out_bias_ref[1, pl.ds(l, 1)], told=ODD_FIRST)

        @pl.when(odd)
        def _():
            load('fc1', l).wait()
            load('fc2', l).wait()

            @pl.when(l == 0)
            def _():
                for c in pairs:
                    c.wait_recv()

            block(ph + 2, mlp)

        reduce(ph + 2, out_bias_ref[2, pl.ds(l, 1)], summed=ODD_FIRST)
        return carry

    lax.fori_loop(0, LAYERS, layer, 0)

    def drain(ph, mlp_in=False, mlp_out=False):
        for g in range(2):
            @pl.when((me != OWNERS[g]) & (odd if mlp_out else True))
            def _():
                rs_copy(ph, g, me).wait_send()

        @pl.when(is_owner)
        def _():
            for d in others(my_group, ODD_FIRST if mlp_in else NEAR_FIRST):
                ag_copy(ph, my_group, d).wait_send()

    @pl.when(jnp.logical_not(odd))
    def _():
        for c in pairs:
            c.wait_send()

    drain(0)

    def drain_layer(l, carry):
        drain(3 * l + 1)
        drain(3 * l + 2, mlp_in=True)
        return carry

    lax.fori_loop(0, LAYERS, drain_layer, 0)
    last = N_PHASES - 1
    for ph in range(3, last, 3):
        drain(ph, mlp_out=True)
    table_load.wait()
    h_out[...] = jnp.concatenate([receive(last, 0), receive(last, 1)], axis=0)
    drain(last, mlp_out=True)


def run_core(emb, pos, posn, in_bias, out_bias, b_fc1, ln_layers, ln_final, table, sk, sv, ck, cv, wqkv, wcq, wout, wfc1, wfc2):
    vm = pl.BlockSpec(memory_space=pltpu.VMEM)
    hbm = pl.BlockSpec(memory_space=pltpu.HBM)
    d_model = emb.shape[-1]
    ln_rows = ln_layers.shape[0] + 1
    return pl.pallas_call(
        core_kernel,
        out_shape=(pltpu.VMEM((BATCH, d_model), BF16),) + tuple(pltpu.VMEM(a.shape, BF16) for a in (table, sk, sv)),
        in_specs=[vm] * 3 + [hbm] * 15,
        out_specs=(vm,) * 4,
        scratch_shapes=[pltpu.VMEM(a.shape[1:], BF16) for a in (ck, cv)]
        + [pltpu.VMEM(a.shape, BF16) for a in (wqkv, wcq, wout, wfc1, wfc2, wfc1, wfc2)]
        + [pltpu.VMEM(b_fc1.shape, F32)]
        + [pltpu.VMEM(a.shape, F32) for a in (in_bias, out_bias, b_fc1)]
        + [pltpu.VMEM((ln_rows, 2, d_model), F32),
           pltpu.VMEM((N_TP, ROWS, d_model), BF16),
           pltpu.VMEM((N_PHASES - 1, 2, ROWS, d_model), F32),
           pltpu.VMEM((N_PHASES - 1, N_TP, ROWS, d_model), F32),
           pltpu.VMEM((N_PHASES, 2, ROWS, d_model), BF16),
           pltpu.VMEM((ROWS, d_model), F32),
           pltpu.VMEM((2, 2, ROWS, HD), F32),
           pltpu.SemaphoreType.DMA((6,)),
           pltpu.SemaphoreType.DMA((7, LAYERS)),
           pltpu.SemaphoreType.DMA((2, 2)),
           pltpu.SemaphoreType.DMA((5,)),
           pltpu.SemaphoreType.DMA((5,)),
           pltpu.SemaphoreType.DMA((N_PHASES, 2)),
           pltpu.SemaphoreType.DMA((N_PHASES, N_TP)),
           pltpu.SemaphoreType.DMA((N_PHASES, N_TP)),
           pltpu.SemaphoreType.DMA((N_PHASES, 2))],
        compiler_params=pltpu.CompilerParams(collective_id=0, has_side_effects=True, vmem_limit_bytes=CORE_VMEM),
        cost_estimate=pl.CostEstimate(flops=4 << 30, bytes_accessed=150 << 20, transcendentals=0),
        name='decode_layers',
    )(emb, pos, posn, *in_hbm(in_bias, out_bias, b_fc1, ln_layers, ln_final, table, sk, sv, ck, cv, wqkv, wcq, wout, wfc1, wfc2))


def gather_kernel(tok_hbm, posn_hbm, table_hbm, pos_hbm, emb_out, pos_out, posn_out, emb_buf, pos_buf, tok_ref, pos_ref, sems, idx_sems):
    idx = [pltpu.make_async_copy(tok_hbm, tok_ref, idx_sems.at[0]), pltpu.make_async_copy(posn_hbm, pos_ref, idx_sems.at[1])]
    for c in idx:
        c.start()
    for c in idx:
        c.wait()
    shard_rows = table_hbm.shape[0]
    base = lax.axis_index('tp') * shard_rows
    copies = []
    for b in range(BATCH):
        row = jnp.clip(tok_ref[b] - base, 0, shard_rows - 1)
        at = pl.multiple_of((row // 8) * 8, 8)
        copies.append(pltpu.make_async_copy(table_hbm.at[pl.ds(at, 8)], emb_buf.at[pl.ds(b * 8, 8)], sems.at[0, b]))
        at = pl.multiple_of((pos_ref[b] // 8) * 8, 8)
        copies.append(pltpu.make_async_copy(pos_hbm.at[pl.ds(at, 8)], pos_buf.at[pl.ds(b * 8, 8)], sems.at[1, b]))
    for c in copies:
        c.start()
    row_i = lax.broadcasted_iota(jnp.int32, (BATCH, 8 * BATCH), 0)
    lane_i = lax.broadcasted_iota(jnp.int32, (BATCH, 8 * BATCH), 1)
    tok_at = jnp.zeros((BATCH, 8 * BATCH), jnp.int32)
    pos_at = jnp.zeros((BATCH, 8 * BATCH), jnp.int32)
    posn_row = lax.broadcasted_iota(jnp.int32, (BATCH, posn_out.shape[2]), 0)
    posn = jnp.zeros(posn_row.shape, jnp.int32)
    for b in range(BATCH):
        row = tok_ref[b] - base
        owned = (row >= 0) & (row < shard_rows)
        tok_at = jnp.where(row_i == b, jnp.where(owned, b * 8 + row % 8, -1), tok_at)
        pos_at = jnp.where(row_i == b, b * 8 + pos_ref[b] % 8, pos_at)
        posn = jnp.where(posn_row == b, pos_ref[b], posn)
    for g in range(2):
        posn_out[g] = jnp.concatenate([posn[g * ROWS:(g + 1) * ROWS]] * HEADS, axis=0)
    pick_tok = jnp.where(lane_i == tok_at, 1.0, 0.0).astype(BF16)
    pick_pos = jnp.where(lane_i == pos_at, 1.0, 0.0).astype(BF16)
    for c in copies:
        c.wait()
    emb = dot(pick_tok, emb_buf[...]).astype(BF16)
    pos = dot(pick_pos, pos_buf[...]).astype(BF16)
    for g in range(2):
        emb_out[g] = emb[g * ROWS:(g + 1) * ROWS]
        pos_out[g] = pos[g * ROWS:(g + 1) * ROWS]


def run_gather(tokens, positions, embed_table, pos_table, time):
    vm = pl.BlockSpec(memory_space=pltpu.VMEM)
    hbm = pl.BlockSpec(memory_space=pltpu.HBM)
    d_model = embed_table.shape[1]
    rows = pltpu.VMEM((2, ROWS, d_model), BF16)
    return pl.pallas_call(
        gather_kernel,
        out_shape=(rows, rows, pltpu.VMEM((2, HEADS * ROWS, time), jnp.int32)),
        in_specs=[hbm] * 4,
        out_specs=(vm, vm, vm),
        scratch_shapes=[pltpu.VMEM((8 * BATCH, d_model), BF16), pltpu.VMEM((8 * BATCH, d_model), BF16),
                        pltpu.SMEM((BATCH,), jnp.int32), pltpu.SMEM((BATCH,), jnp.int32),
                        pltpu.SemaphoreType.DMA((2, BATCH)), pltpu.SemaphoreType.DMA((2,))],
        compiler_params=pltpu.CompilerParams(vmem_limit_bytes=GATHER_VMEM),
        name='gather_rows',
    )(*in_hbm(tokens, positions, embed_table, pos_table))


N_TILES = 3


def final_kernel(h_ref, table_ref, sk_ref, sv_ref, logits_ref, sk_out, sv_out, sems):
    copies = [pltpu.make_async_copy(sk_ref, sk_out, sems.at[0]), pltpu.make_async_copy(sv_ref, sv_out, sems.at[1])]
    for c in copies:
        c.start()
    h_t = h_ref[...].astype(F32).T.astype(BF16)
    tile = table_ref.shape[0] // N_TILES
    for i in range(N_TILES):
        logits_ref[:, i * tile:(i + 1) * tile] = dot(table_ref[i * tile:(i + 1) * tile], h_t).T
    for c in copies:
        c.wait()


def run_final(hidden, table, sk, sv):
    vm = pl.BlockSpec(memory_space=pltpu.VMEM)
    hbm = pl.BlockSpec(memory_space=pltpu.HBM)
    cache = jax.ShapeDtypeStruct(sk.shape, BF16)
    return pl.pallas_call(
        final_kernel,
        out_shape=(jax.ShapeDtypeStruct((BATCH, table.shape[0]), F32), cache, cache),
        in_specs=[vm] * 4,
        out_specs=(vm, hbm, hbm),
        scratch_shapes=[pltpu.SemaphoreType.DMA((2,))],
        compiler_params=pltpu.CompilerParams(vmem_limit_bytes=FINAL_VMEM),
        name='logits_and_caches',
    )(hidden, table, sk, sv)


def solution(mesh):
    def local_step(tokens, positions, self_keys, self_vals, cross_keys, cross_vals, embed_table, pos_table, w_qkv, w_cq, in_bias, w_out, out_bias, w_fc1, b_fc1, w_fc2, ln_layers, ln_final):
        d_model = embed_table.shape[1]

        def rows_by_time(cache):
            return jnp.transpose(cache, (0, 1, 3, 4, 2)).reshape(LAYERS, BATCH * HD, cache.shape[2])

        def as_cache(rows):
            return jnp.transpose(rows.reshape(LAYERS, BATCH, HEADS, HEAD_DIM, rows.shape[2]), (0, 1, 4, 2, 3))

        sk, sv = rows_by_time(self_keys), rows_by_time(self_vals)
        emb, pos, posn = run_gather(tokens, positions, embed_table, pos_table, sk.shape[2])
        hidden, table, sk, sv = run_core(
            emb, pos, posn, in_bias, jnp.transpose(out_bias, (1, 0, 2)), b_fc1, ln_layers.reshape(-1, 2, d_model), ln_final[None],
            embed_table, sk, sv, rows_by_time(cross_keys), rows_by_time(cross_vals),
            jnp.transpose(w_qkv, (0, 2, 3, 4, 1)).reshape(LAYERS, 3 * HD, d_model),
            jnp.transpose(w_cq, (0, 2, 3, 1)).reshape(LAYERS, HD, d_model),
            w_out.reshape(LAYERS, 2, HD, d_model), w_fc1, w_fc2)
        logits, new_sk, new_sv = run_final(hidden, table, sk, sv)
        return logits, as_cache(new_sk), as_cache(new_sv)

    batch_spec = P('dp')
    cache_spec = P(None, 'dp', None, 'tp', None)
    in_specs = (batch_spec, batch_spec, cache_spec, cache_spec, cache_spec, cache_spec, P('tp', None), P(None, None), P(None, None, None, 'tp', None), P(None, None, 'tp', None), P(None, None, 'tp', None), P(None, None, 'tp', None, None), P(None, None, None), P(None, None, 'tp'), P(None, 'tp'), P(None, 'tp', None), P(None, None, None, None), P(None, None))
    out_specs = (P('dp', 'tp'), cache_spec, cache_spec)
    return jax.shard_map(local_step, mesh=mesh, in_specs=in_specs, out_specs=out_specs, check_vma=False)
```

```python
import functools

import jax
import jax.numpy as jnp
from jax import lax
from jax.experimental import pallas as pl
from jax.experimental.pallas import tpu as pltpu
from jax.sharding import PartitionSpec as P

BF16 = jnp.bfloat16
F32 = jnp.float32
MESH = pl.DeviceIdType.MESH
N_TP = 8
OWNERS = (3, 5)
NEAR_FIRST = (2, 1, 0, 5, 4, 7, 6)
ODD_FIRST = (1, 5, 7)
ROWS = 8
BATCH = 16
HEADS = 2
HEAD_DIM = 64
HD = HEADS * HEAD_DIM
LAYERS = 2
GROUP_ROWS = 8 * 128
N_PHASES = 1 + 3 * LAYERS
CORE_VMEM = 32 << 20
GATHER_VMEM = 4 << 20
FINAL_VMEM = 6 << 20
NEG = -1e30


def dot(a, b):
    return jnp.dot(a, b, preferred_element_type=F32)


def dot_nt(a, b):
    return lax.dot_general(a, b, (((1,), (1,)), ((), ())), preferred_element_type=F32)


def in_hbm(*arrays):
    return tuple(pltpu.with_memory_space_constraint(a, pltpu.HBM) for a in arrays)


def layer_norm(x, gain, shift):
    mean = jnp.mean(x, axis=-1, keepdims=True)
    centred = x - mean
    var = jnp.mean(centred * centred, axis=-1, keepdims=True)
    return (centred * lax.rsqrt(var + 1e-5) * gain + shift).astype(BF16)


def head_row(ref, *idx):
    v = ref[idx]
    return jnp.concatenate([v[0:1], v[1:2]], axis=1)


def spread_queries(q):
    q2 = jnp.concatenate([q, q], axis=0)
    row = lax.broadcasted_iota(jnp.int32, q2.shape, 0)
    lane = lax.broadcasted_iota(jnp.int32, q2.shape, 1)
    q2 = jnp.where((row // ROWS) == (lane // HEAD_DIM), q2, 0.0)
    rb = row % ROWS
    return jnp.concatenate([jnp.where(rb == b, q2, 0.0).astype(BF16) for b in range(ROWS)], axis=1)


def gather_heads(mixed):
    row = lax.broadcasted_iota(jnp.int32, (HEADS * ROWS, HD), 0) % ROWS
    acc = jnp.zeros(row.shape, F32)
    for b in range(ROWS):
        acc = jnp.where(row == b, mixed[:, b * HD:(b + 1) * HD], acc)
    lane = lax.broadcasted_iota(jnp.int32, (ROWS, HD), 1)
    return jnp.where(lane < HEAD_DIM, acc[:ROWS], acc[ROWS:])


def core_kernel(emb_ref, pos_ref, posn_ref, in_bias_hbm, out_bias_hbm, b_fc1_hbm, ln_hbm, lnf_hbm,
                table_hbm, sk_hbm, sv_hbm, ck_hbm, cv_hbm, wqkv_hbm, wcq_hbm, wout_hbm, wfc1_hbm, wfc2_hbm,
                h_out, table, sk, sv,
                ck, cv, wqkv, wcq, wout, wfc1, wfc2, pair_fc1, pair_fc2, pair_b,
                in_bias_ref, out_bias_ref, b_fc1_ref, ln_ref,
                emb_rs, part_send, part_rs, hbuf, x_ref, new_ref,
                small_sems, load_sems, half_sems, pair_send, pair_recv, rs_send, rs_recv, ag_send, ag_recv):
    me = lax.axis_index('tp')
    n_ln = ln_hbm.shape[0]
    smalls = [(in_bias_hbm, in_bias_ref), (out_bias_hbm, out_bias_ref), (b_fc1_hbm, b_fc1_ref),
              (ln_hbm, ln_ref.at[pl.ds(0, n_ln)]), (lnf_hbm, ln_ref.at[pl.ds(n_ln, 1)])]
    small_loads = [pltpu.make_async_copy(src, dst, small_sems.at[i]) for i, (src, dst) in enumerate(smalls)]
    table_load = pltpu.make_async_copy(table_hbm, table, small_sems.at[len(smalls)])
    refs = {'wqkv': (wqkv_hbm, wqkv), 'sk': (sk_hbm, sk), 'sv': (sv_hbm, sv), 'wout': (wout_hbm, wout),
            'wcq': (wcq_hbm, wcq), 'fc1': (wfc1_hbm, wfc1), 'fc2': (wfc2_hbm, wfc2)}

    def load(name, l):
        src, dst = refs[name]
        return pltpu.make_async_copy(src.at[l], dst.at[l], load_sems.at[list(refs).index(name), l])

    def rows_of(g):
        return pl.ds(pl.multiple_of(g * GROUP_ROWS, GROUP_ROWS), GROUP_ROWS)

    def load_half(i, l, g):
        src, dst = ((ck_hbm, ck), (cv_hbm, cv))[i]
        return pltpu.make_async_copy(src.at[l, rows_of(g)], dst.at[rows_of(g)], half_sems.at[i, g])

    for c in small_loads:
        c.start()
    odd = me % 2 == 1

    barrier = pltpu.get_barrier_semaphore()
    is_owner = (me == OWNERS[0]) | (me == OWNERS[1])
    for d in range(N_TP):
        @pl.when((me != d) if d in OWNERS else is_owner)
        def _():
            pl.semaphore_signal(barrier, inc=1, device_id={'tp': d}, device_id_type=MESH)

    @pl.when(odd & jnp.logical_not(is_owner))
    def _():
        pl.semaphore_signal(barrier, inc=1, device_id={'tp': me - 1}, device_id_type=MESH)

    @pl.when(is_owner)
    def _():
        pl.semaphore_wait(barrier, N_TP - 1)

    @pl.when(odd & jnp.logical_not(is_owner))
    def _():
        pl.semaphore_wait(barrier, 2)

    alone = jnp.logical_not(odd) & (me != OWNERS[0] - 1) & (me != OWNERS[1] - 1)

    @pl.when(alone)
    def _():
        pl.semaphore_wait(barrier, 3)

    @pl.when(jnp.logical_not(odd) & jnp.logical_not(alone))
    def _():
        pl.semaphore_wait(barrier, 2)

    def owner_of(g):
        return OWNERS[0] + (OWNERS[1] - OWNERS[0]) * g

    def others(g, of=NEAR_FIRST):
        return [d + g * (N_TP - 2 - 2 * (d // 2) + d % 2 - d) for d in of]

    def rs_copy(ph, g, i):
        if isinstance(ph, int) and ph == 0:
            src, dst = emb_ref.at[g], emb_rs.at[i]
        else:
            src, dst = part_send.at[ph - 1, g], part_rs.at[ph - 1, i]
        return pltpu.make_async_remote_copy(src_ref=src, dst_ref=dst, send_sem=rs_send.at[ph, g], recv_sem=rs_recv.at[ph, i],
                                            device_id={'tp': owner_of(g)}, device_id_type=MESH)

    def ag_copy(ph, g, d):
        return pltpu.make_async_remote_copy(src_ref=hbuf.at[ph, g], dst_ref=hbuf.at[ph, g], send_sem=ag_send.at[ph, d], recv_sem=ag_recv.at[ph, g],
                                            device_id={'tp': d}, device_id_type=MESH)

    def send(ph, g):
        @pl.when(me != owner_of(g))
        def _():
            rs_copy(ph, g, me).start()

    my_group = (me - OWNERS[0]) // (OWNERS[1] - OWNERS[0])

    def reduce(ph, bias, summed=NEAR_FIRST, told=NEAR_FIRST):
        @pl.when(is_owner)
        def _():
            g = my_group
            first = bias is None
            total = (emb_ref[g] if first else part_send[ph - 1, g]).astype(F32)
            base = pos_ref[g].astype(F32) if first else x_ref[...] + bias
            for i in others(g, summed):
                rs_copy(ph, g, i).wait_recv()
                total = total + (emb_rs[i] if first else part_rs[ph - 1, i]).astype(F32)
            x = total.astype(BF16).astype(F32) + base
            hbuf[ph, g] = layer_norm(x, ln_ref[ph, 0:1], ln_ref[ph, 1:2])
            for d in reversed(others(g, told)):
                ag_copy(ph, g, d).start()
            x_ref[...] = x

    pairs = [pltpu.make_async_remote_copy(src_ref=src, dst_ref=dst, send_sem=pair_send.at[i], recv_sem=pair_recv.at[i],
                                          device_id={'tp': jnp.minimum(me + 1, N_TP - 1)}, device_id_type=MESH)
             for i, (src, dst) in enumerate([(wfc1_hbm.at[0], pair_fc1.at[0]), (wfc2_hbm.at[0], pair_fc2.at[0]), (b_fc1_hbm, pair_b),
                                             (wfc1_hbm.at[1], pair_fc1.at[1]), (wfc2_hbm.at[1], pair_fc2.at[1])])]

    def receive(ph, g):
        @pl.when(me != owner_of(g))
        def _():
            ag_copy(ph, g, 0).wait_recv()
        return hbuf[ph, g]

    for g in range(2):
        send(0, g)

    @pl.when(jnp.logical_not(odd))
    def _():
        for c in pairs:
            c.start()

    for name in ('wqkv', 'sk', 'sv', 'wout', 'wcq'):
        load(name, 0).start()
    for g in range(2):
        for i in range(2):
            load_half(i, 0, g).start()
    @pl.when(odd)
    def _():
        for name in ('fc1', 'fc2'):
            load(name, 0).start()

    for c in small_loads:
        c.wait()
    reduce(0, None)

    time = sk.shape[2]
    qk_scale = HEAD_DIM ** -0.5

    def attend_self(l, g, hidden):
        qkv = dot_nt(hidden, wqkv[l])
        q = (qkv[:, :HD] + head_row(in_bias_ref, l, 0)).astype(BF16).astype(F32)
        k_new = qkv[:, HD:2 * HD].astype(BF16).astype(F32)
        v_new = (qkv[:, 2 * HD:] + head_row(in_bias_ref, l, 1)).astype(BF16).astype(F32)
        new_ref[0, g] = k_new
        new_ref[1, g] = v_new
        prod = q * k_new
        s_new = jnp.concatenate([jnp.sum(prod[:, :HEAD_DIM], axis=1, keepdims=True), jnp.sum(prod[:, HEAD_DIM:], axis=1, keepdims=True)], axis=0)
        posn = posn_ref[g]
        t_idx = lax.broadcasted_iota(jnp.int32, posn.shape, 1)
        here = t_idx == posn
        s = jnp.where(here, s_new, dot(spread_queries(q), sk[l, rows_of(g)])) * qk_scale
        s = jnp.where(t_idx <= posn, s, NEG)
        e = jnp.exp(s - jnp.max(s, axis=-1, keepdims=True))
        w = (e / jnp.sum(e, axis=-1, keepdims=True)).astype(BF16).astype(F32)
        w_new = jnp.sum(jnp.where(here, w, 0.0), axis=-1, keepdims=True)
        w_old = jnp.where(here, 0.0, w)
        mixed = gather_heads(dot_nt(w_old.astype(BF16), sv[l, rows_of(g)]))
        lane = lax.broadcasted_iota(jnp.int32, (ROWS, HD), 1)
        w_row = jnp.where(lane < HEAD_DIM, w_new[:ROWS], w_new[ROWS:])
        o = (mixed + w_row * v_new).astype(BF16)
        return dot(o, wout[l, 0])

    def write_new(l, g):
        t_row = lax.broadcasted_iota(jnp.int32, (HD, time), 1)
        cols = [new_ref[i, g].T for i in range(2)]
        for b in range(ROWS):
            at = t_row == posn_ref[g, b:b + 1]
            rows = pl.ds(pl.multiple_of(g * GROUP_ROWS + b * HD, HD), HD)
            for ref, col in zip((sk, sv), cols):
                ref[l, rows] = jnp.where(at, col[:, b:b + 1], ref[l, rows].astype(F32)).astype(BF16)

    def attend_cross(l, g, hidden):
        q = (dot_nt(hidden, wcq[l]) + head_row(in_bias_ref, l, 2)).astype(BF16).astype(F32)
        load_half(0, l, g).wait()
        s = dot(spread_queries(q), ck[rows_of(g)]) * qk_scale
        e = jnp.exp(s - jnp.max(s, axis=-1, keepdims=True))
        w = e / jnp.sum(e, axis=-1, keepdims=True)
        load_half(1, l, g).wait()
        o = gather_heads(dot_nt(w.astype(BF16), cv[rows_of(g)])).astype(BF16)
        return dot(o, wout[l, 1])

    def mlp(l, g, hidden):
        part = None
        for fc1, b, fc2 in ((wfc1, b_fc1_ref, wfc2), (pair_fc1, pair_b, pair_fc2)):
            f = dot(hidden, fc1[l]) + b[pl.ds(l, 1)]
            act = (f * 0.5 * (1.0 + lax.erf(f * (2.0 ** -0.5)))).astype(BF16)
            half = dot(act, fc2[l])
            part = half if part is None else part + half
        return part

    def both_streams(body):
        lax.fori_loop(0, 2, lambda g, c: (body(g), c)[1], 0)

    def layer(l, carry):
        ph = 3 * l + 1

        def block(ph, compute, after=None):
            def stream(g):
                part_send[ph - 1, g] = compute(l, g, receive(ph - 1, g))
                send(ph, g)
                if after is not None:
                    after(g)
            both_streams(stream)

        for name in ('wqkv', 'sk', 'sv', 'wout'):
            load(name, l).wait()
        block(ph, attend_self)
        reduce(ph, out_bias_ref[0, pl.ds(l, 1)])

        @pl.when(l == 0)
        def _():
            for name in ('wqkv', 'sk', 'sv', 'wout', 'wcq'):
                load(name, 1).start()
            table_load.start()

            @pl.when(odd)
            def _():
                for name in ('fc1', 'fc2'):
                    load(name, 1).start()

        both_streams(lambda g: write_new(l, g))
        load('wcq', l).wait()

        def next_half(g):
            @pl.when(l + 1 < LAYERS)
            def _():
                for i in range(2):
                    load_half(i, l + 1, g).start()

        block(ph + 1, attend_cross, next_half)
        reduce(ph + 1, out_bias_ref[1, pl.ds(l, 1)], told=ODD_FIRST)

        @pl.when(odd)
        def _():
            load('fc1', l).wait()
            load('fc2', l).wait()

            @pl.when(l == 0)
            def _():
                for c in pairs:
                    c.wait_recv()

            block(ph + 2, mlp)

        reduce(ph + 2, out_bias_ref[2, pl.ds(l, 1)], summed=ODD_FIRST)
        return carry

    lax.fori_loop(0, LAYERS, layer, 0)

    def drain(ph, mlp_in=False, mlp_out=False):
        for g in range(2):
            @pl.when((me != OWNERS[g]) & (odd if mlp_out else True))
            def _():
                rs_copy(ph, g, me).wait_send()

        @pl.when(is_owner)
        def _():
            for d in others(my_group, ODD_FIRST if mlp_in else NEAR_FIRST):
                ag_copy(ph, my_group, d).wait_send()

    @pl.when(jnp.logical_not(odd))
    def _():
        for c in pairs:
            c.wait_send()

    drain(0)

    def drain_layer(l, carry):
        drain(3 * l + 1)
        drain(3 * l + 2, mlp_in=True)
        return carry

    lax.fori_loop(0, LAYERS, drain_layer, 0)
    last = N_PHASES - 1
    for ph in range(3, last, 3):
        drain(ph, mlp_out=True)
    table_load.wait()
    h_out[...] = jnp.concatenate([receive(last, 0), receive(last, 1)], axis=0)
    drain(last, mlp_out=True)


def run_core(emb, pos, posn, in_bias, out_bias, b_fc1, ln_layers, ln_final, table, sk, sv, ck, cv, wqkv, wcq, wout, wfc1, wfc2):
    vm = pl.BlockSpec(memory_space=pltpu.VMEM)
    hbm = pl.BlockSpec(memory_space=pltpu.HBM)
    d_model = emb.shape[-1]
    ln_rows = ln_layers.shape[0] + 1
    return pl.pallas_call(
        core_kernel,
        out_shape=(pltpu.VMEM((BATCH, d_model), BF16),) + tuple(pltpu.VMEM(a.shape, BF16) for a in (table, sk, sv)),
        in_specs=[vm] * 3 + [hbm] * 15,
        out_specs=(vm,) * 4,
        scratch_shapes=[pltpu.VMEM(a.shape[1:], BF16) for a in (ck, cv)]
        + [pltpu.VMEM(a.shape, BF16) for a in (wqkv, wcq, wout, wfc1, wfc2, wfc1, wfc2)]
        + [pltpu.VMEM(b_fc1.shape, F32)]
        + [pltpu.VMEM(a.shape, F32) for a in (in_bias, out_bias, b_fc1)]
        + [pltpu.VMEM((ln_rows, 2, d_model), F32),
           pltpu.VMEM((N_TP, ROWS, d_model), BF16),
           pltpu.VMEM((N_PHASES - 1, 2, ROWS, d_model), F32),
           pltpu.VMEM((N_PHASES - 1, N_TP, ROWS, d_model), F32),
           pltpu.VMEM((N_PHASES, 2, ROWS, d_model), BF16),
           pltpu.VMEM((ROWS, d_model), F32),
           pltpu.VMEM((2, 2, ROWS, HD), F32),
           pltpu.SemaphoreType.DMA((6,)),
           pltpu.SemaphoreType.DMA((7, LAYERS)),
           pltpu.SemaphoreType.DMA((2, 2)),
           pltpu.SemaphoreType.DMA((5,)),
           pltpu.SemaphoreType.DMA((5,)),
           pltpu.SemaphoreType.DMA((N_PHASES, 2)),
           pltpu.SemaphoreType.DMA((N_PHASES, N_TP)),
           pltpu.SemaphoreType.DMA((N_PHASES, N_TP)),
           pltpu.SemaphoreType.DMA((N_PHASES, 2))],
        compiler_params=pltpu.CompilerParams(collective_id=0, has_side_effects=True, vmem_limit_bytes=CORE_VMEM),
        cost_estimate=pl.CostEstimate(flops=4 << 30, bytes_accessed=150 << 20, transcendentals=0),
        name='decode_layers',
    )(emb, pos, posn, *in_hbm(in_bias, out_bias, b_fc1, ln_layers, ln_final, table, sk, sv, ck, cv, wqkv, wcq, wout, wfc1, wfc2))


def gather_kernel(tok_hbm, posn_hbm, table_hbm, pos_hbm, emb_out, pos_out, posn_out, emb_buf, pos_buf, tok_ref, pos_ref, sems, idx_sems):
    idx = [pltpu.make_async_copy(tok_hbm, tok_ref, idx_sems.at[0]), pltpu.make_async_copy(posn_hbm, pos_ref, idx_sems.at[1])]
    for c in idx:
        c.start()
    for c in idx:
        c.wait()
    shard_rows = table_hbm.shape[0]
    base = lax.axis_index('tp') * shard_rows
    copies = []
    for b in range(BATCH):
        row = jnp.clip(tok_ref[b] - base, 0, shard_rows - 1)
        at = pl.multiple_of((row // 8) * 8, 8)
        copies.append(pltpu.make_async_copy(table_hbm.at[pl.ds(at, 8)], emb_buf.at[pl.ds(b * 8, 8)], sems.at[0, b]))
        at = pl.multiple_of((pos_ref[b] // 8) * 8, 8)
        copies.append(pltpu.make_async_copy(pos_hbm.at[pl.ds(at, 8)], pos_buf.at[pl.ds(b * 8, 8)], sems.at[1, b]))
    for c in copies:
        c.start()
    row_i = lax.broadcasted_iota(jnp.int32, (BATCH, 8 * BATCH), 0)
    lane_i = lax.broadcasted_iota(jnp.int32, (BATCH, 8 * BATCH), 1)
    tok_at = jnp.zeros((BATCH, 8 * BATCH), jnp.int32)
    pos_at = jnp.zeros((BATCH, 8 * BATCH), jnp.int32)
    posn_row = lax.broadcasted_iota(jnp.int32, (BATCH, posn_out.shape[2]), 0)
    posn = jnp.zeros(posn_row.shape, jnp.int32)
    for b in range(BATCH):
        row = tok_ref[b] - base
        owned = (row >= 0) & (row < shard_rows)
        tok_at = jnp.where(row_i == b, jnp.where(owned, b * 8 + row % 8, -1), tok_at)
        pos_at = jnp.where(row_i == b, b * 8 + pos_ref[b] % 8, pos_at)
        posn = jnp.where(posn_row == b, pos_ref[b], posn)
    for g in range(2):
        posn_out[g] = jnp.concatenate([posn[g * ROWS:(g + 1) * ROWS]] * HEADS, axis=0)
    pick_tok = jnp.where(lane_i == tok_at, 1.0, 0.0).astype(BF16)
    pick_pos = jnp.where(lane_i == pos_at, 1.0, 0.0).astype(BF16)
    for c in copies:
        c.wait()
    emb = dot(pick_tok, emb_buf[...]).astype(BF16)
    pos = dot(pick_pos, pos_buf[...]).astype(BF16)
    for g in range(2):
        emb_out[g] = emb[g * ROWS:(g + 1) * ROWS]
        pos_out[g] = pos[g * ROWS:(g + 1) * ROWS]


def run_gather(tokens, positions, embed_table, pos_table, time):
    vm = pl.BlockSpec(memory_space=pltpu.VMEM)
    hbm = pl.BlockSpec(memory_space=pltpu.HBM)
    d_model = embed_table.shape[1]
    rows = pltpu.VMEM((2, ROWS, d_model), BF16)
    return pl.pallas_call(
        gather_kernel,
        out_shape=(rows, rows, pltpu.VMEM((2, HEADS * ROWS, time), jnp.int32)),
        in_specs=[hbm] * 4,
        out_specs=(vm, vm, vm),
        scratch_shapes=[pltpu.VMEM((8 * BATCH, d_model), BF16), pltpu.VMEM((8 * BATCH, d_model), BF16),
                        pltpu.SMEM((BATCH,), jnp.int32), pltpu.SMEM((BATCH,), jnp.int32),
                        pltpu.SemaphoreType.DMA((2, BATCH)), pltpu.SemaphoreType.DMA((2,))],
        compiler_params=pltpu.CompilerParams(vmem_limit_bytes=GATHER_VMEM),
        name='gather_rows',
    )(*in_hbm(tokens, positions, embed_table, pos_table))


N_TILES = 3


def final_kernel(h_ref, table_ref, sk_ref, sv_ref, logits_ref, sk_out, sv_out, sems):
    copies = [pltpu.make_async_copy(sk_ref, sk_out, sems.at[0]), pltpu.make_async_copy(sv_ref, sv_out, sems.at[1])]
    for c in copies:
        c.start()
    h_t = h_ref[...].astype(F32).T.astype(BF16)
    tile = table_ref.shape[0] // N_TILES
    for i in range(N_TILES):
        logits_ref[:, i * tile:(i + 1) * tile] = dot(table_ref[i * tile:(i + 1) * tile], h_t).T
    for c in copies:
        c.wait()


def run_final(hidden, table, sk, sv):
    vm = pl.BlockSpec(memory_space=pltpu.VMEM)
    hbm = pl.BlockSpec(memory_space=pltpu.HBM)
    cache = jax.ShapeDtypeStruct(sk.shape, BF16)
    return pl.pallas_call(
        final_kernel,
        out_shape=(jax.ShapeDtypeStruct((BATCH, table.shape[0]), F32), cache, cache),
        in_specs=[vm] * 4,
        out_specs=(vm, hbm, hbm),
        scratch_shapes=[pltpu.SemaphoreType.DMA((2,))],
        compiler_params=pltpu.CompilerParams(vmem_limit_bytes=FINAL_VMEM),
        name='logits_and_caches',
    )(hidden, table, sk, sv)


def solution(mesh):
    def local_step(tokens, positions, self_keys, self_vals, cross_keys, cross_vals, embed_table, pos_table, w_qkv, w_cq, in_bias, w_out, out_bias, w_fc1, b_fc1, w_fc2, ln_layers, ln_final):
        d_model = embed_table.shape[1]

        def rows_by_time(cache):
            return jnp.transpose(cache, (0, 1, 3, 4, 2)).reshape(LAYERS, BATCH * HD, cache.shape[2])

        def as_cache(rows):
            return jnp.transpose(rows.reshape(LAYERS, BATCH, HEADS, HEAD_DIM, rows.shape[2]), (0, 1, 4, 2, 3))

        sk, sv = rows_by_time(self_keys), rows_by_time(self_vals)
        emb, pos, posn = run_gather(tokens, positions, embed_table, pos_table, sk.shape[2])
        hidden, table, sk, sv = run_core(
            emb, pos, posn, in_bias, jnp.transpose(out_bias, (1, 0, 2)), b_fc1, ln_layers.reshape(-1, 2, d_model), ln_final[None],
            embed_table, sk, sv, rows_by_time(cross_keys), rows_by_time(cross_vals),
            jnp.transpose(w_qkv, (0, 2, 3, 4, 1)).reshape(LAYERS, 3 * HD, d_model),
            jnp.transpose(w_cq, (0, 2, 3, 1)).reshape(LAYERS, HD, d_model),
            w_out.reshape(LAYERS, 2, HD, d_model), w_fc1, w_fc2)
        logits, new_sk, new_sv = run_final(hidden, table, sk, sv)
        return logits, as_cache(new_sk), as_cache(new_sv)

    batch_spec = P('dp')
    cache_spec = P(None, 'dp', None, 'tp', None)
    in_specs = (batch_spec, batch_spec, cache_spec, cache_spec, cache_spec, cache_spec, P('tp', None), P(None, None), P(None, None, None, 'tp', None), P(None, None, 'tp', None), P(None, None, 'tp', None), P(None, None, 'tp', None, None), P(None, None, None), P(None, None, 'tp'), P(None, 'tp'), P(None, 'tp', None), P(None, None, None, None), P(None, None))
    out_specs = (P('dp', 'tp'), cache_spec, cache_spec)
    return jax.shard_map(local_step, mesh=mesh, in_specs=in_specs, out_specs=out_specs, check_vma=False)
```
